32 devices in a mesh: seq: 8 (over z, y), head: 4 (over x, core).
Axes of the slice: x: 2, y: 2, z: 4, core: 2. Of those that a mesh axis runs over, the one named last changes fastest.
Arguments:
- hidden: bfloat16 [4096, 8192], P('seq', 'head'), may hold values from -6 to 6
- gain: float32 [8192], replicated, may hold values from 0.25 to 1.75
- key_matrix: bfloat16 [8192, 512], P(None, 'head'), may hold values from -0.0625 to 0.0625
- value_matrix: bfloat16 [8192, 512], P(None, 'head'), may hold values from -0.0625 to 0.0625
- queries: bfloat16 [64, 4096], P(None, 'head'), may hold values from -360 to 360
- window_len: int32 [4], P('head'), may hold values from 16 to 64, as said below
- kernel_width: int32 [4], P('head'), may hold values from 1 to 15, as said below
- kept_block_count: int32 [4], P('head'), may hold values from 1 to 16
Outputs:
- block_scores: float32 [4, 32], P('head', 'seq')
- kept_fraction: float32 [4], P('head')
The draws below stay inside these ranges and needn't reach their ends.
Inputs may be any that keep to these rules, and one draw needn't show every extreme that they name: `window_len`: at least one key-value head uses all 64 window queries. `kernel_width`: odd; at least one key-value head has width 15.
All inputs are finite; a program needn't handle non-finite values.
Results may differ from the reference program's by a relative error of at most 0.0112.
The reference program's roundings to bfloat16 on the way (of `normed` and `keys`) count: a program that leaves them out, or rounds other values in their place, can miss the bound.
Values may be sent and summed in bfloat16 or wider, within the bound.
No kernel may reach another device: no remote copies, remote signals or barrier semaphores. Data moves between devices by JAX's collectives and lax.ppermute only.
A program may use at most 128 MiB of HBM per device.

```python
import jax
import jax.numpy as jnp
from jax import lax

MODEL_WIDTH = 8192
HEAD_DIMENSION = 128
QUERY_PER_GROUP = 8
WINDOW_QUERIES = 64
BLK = 128
KERNEL_LIMIT = 15
KEY_VALUE_HEADS = 4
H = 32
PROMPT_TOKENS = 4096
KEY_BLOCK_COUNT = 32
N_SEQ = 8


def draw_queries(key, part):
    leading_part = jax.random.fold_in(jax.random.fold_in(key, 7), 0)
    base = jax.random.truncated_normal(leading_part, -6.0, 6.0, (WINDOW_QUERIES, H * HEAD_DIMENSION), jnp.float32)
    return base.astype(jnp.bfloat16)


def draw_window_len(key, part):
    leading_part, trailing_part = jax.random.split(jax.random.fold_in(key, 11))
    value_rows = jax.random.randint(leading_part, (KEY_VALUE_HEADS,), WINDOW_QUERIES // 4, WINDOW_QUERIES + 1)
    selected_blocks = jax.random.randint(trailing_part, (), 0, KEY_VALUE_HEADS)
    return jnp.where(jnp.arange(KEY_VALUE_HEADS) == selected_blocks, WINDOW_QUERIES, value_rows).astype(jnp.int32)


def draw_kernel_width(key, part):
    leading_part, trailing_part = jax.random.split(jax.random.fold_in(key, 13))
    kernel_halfspan = jax.random.randint(leading_part, (KEY_VALUE_HEADS,), 0, (KERNEL_LIMIT - 1) // 2 + 1)
    selected_blocks = jax.random.randint(trailing_part, (), 0, KEY_VALUE_HEADS)
    return jnp.where(jnp.arange(KEY_VALUE_HEADS) == selected_blocks, KERNEL_LIMIT, 2 * kernel_halfspan + 1).astype(jnp.int32)


def set_ends(values, key, smallest, top_value):
    longest = values.shape.index(max(values.shape))
    spots = []
    for shift in (0, 1):
        where = [jax.random.randint(jax.random.fold_in(key, axis), (), 0, length) for axis, length in enumerate(values.shape)]
        where[longest] = (where[longest] + shift) % values.shape[longest]
        spots.append(tuple(where))
    return values.at[spots[0]].set(smallest).at[spots[1]].set(top_value)


def shard_levels(own_key, shape, pieces, least, top_value):
    level = 1.0
    for position, parts in pieces:
        draws = jax.random.uniform(jax.random.fold_in(jax.random.fold_in(own_key, 6), position), (parts,), jnp.float32, least / len(pieces), top_value / len(pieces))
        level = level * jnp.repeat(jnp.exp(draws), shape[position] // parts).reshape((-1,) + (1,) * (len(shape) - 1 - position))
    return level


def scatter_about(rng, shape, spread, most, pieces=(), held_as=jnp.bfloat16):
    drawn = spread * jax.random.normal(rng, shape, jnp.float32)
    if pieces:
        drawn = drawn * shard_levels(rng, shape, pieces, -0.22, 0.18)
    return jnp.clip(drawn, -most, most).astype(held_as)


def setup_inputs(seed: int = 0) -> dict:
    streams_of = jax.random.split(jax.random.key(seed), 9)
    hidden = scatter_about(streams_of[0], (PROMPT_TOKENS, MODEL_WIDTH), 1.0, 6.0, ((0, 8), (1, 4)))
    gain = jnp.clip(1.0 + 0.15 * jax.random.normal(streams_of[1], (MODEL_WIDTH,), jnp.float32), 0.25, 1.75)
    key_matrix = scatter_about(streams_of[2], (MODEL_WIDTH, KEY_VALUE_HEADS * HEAD_DIMENSION), MODEL_WIDTH ** -0.5, 0.0625, ((1, 4),))
    value_matrix = scatter_about(streams_of[3], (MODEL_WIDTH, KEY_VALUE_HEADS * HEAD_DIMENSION), MODEL_WIDTH ** -0.5, 0.0625, ((1, 4),))
    queries = draw_queries(jax.random.fold_in(streams_of[8], 71), 0)
    window_len = draw_window_len(jax.random.fold_in(streams_of[8], 71), 0)
    kernel_width = draw_kernel_width(jax.random.fold_in(streams_of[8], 71), 0)
    kept_block_count = set_ends(jax.random.randint(streams_of[7], (KEY_VALUE_HEADS,), 1, KEY_BLOCK_COUNT // 2 + 1), jax.random.fold_in(streams_of[7], 1), 1, (KEY_BLOCK_COUNT // 2 + 1) - 1).astype(jnp.int32)
    return {"hidden": hidden, "gain": gain, "key_matrix": key_matrix, "value_matrix": value_matrix, "queries": queries, "window_len": window_len, "kernel_width": kernel_width, "kept_block_count": kept_block_count}


def rotate(raw, positions):
    half = raw.shape[1] // 2
    freq = 500000.0 ** (-(jnp.arange(half).astype(jnp.float32) * 2.0) / raw.shape[1])
    angle = positions[:, None] * freq[None, :]
    leading_part = raw[:, :half]
    trailing_part = raw[:, half:]
    return jnp.concatenate([leading_part * jnp.cos(angle) - trailing_part * jnp.sin(angle), trailing_part * jnp.cos(angle) + leading_part * jnp.sin(angle)], axis=1)

def reference(hidden, gain, key_matrix, value_matrix, queries, window_len, kernel_width, kept_block_count):

    def project(rows):
        floats = rows.astype(jnp.float32)
        meansq = lax.optimization_barrier(jnp.mean(floats * floats, axis=1))
        normed = (floats * gain[None, :]).astype(jnp.bfloat16)
        scale = lax.rsqrt(meansq + 1e-05)[:, None]
        kproj = jnp.dot(normed, key_matrix, preferred_element_type=jnp.float32) * scale
        vproj = jnp.dot(normed, value_matrix, preferred_element_type=jnp.float32) * scale
        return (kproj, vproj)
    blocks = hidden.reshape(N_SEQ, PROMPT_TOKENS // N_SEQ, MODEL_WIDTH)
    key_states_full, value_states_full = lax.map(project, blocks)
    key_states_full = key_states_full.reshape(PROMPT_TOKENS, KEY_VALUE_HEADS, HEAD_DIMENSION).transpose(1, 0, 2)
    value_states_full = value_states_full.reshape(PROMPT_TOKENS, KEY_VALUE_HEADS, HEAD_DIMENSION).transpose(1, 0, 2)
    query_states_full = queries.reshape(WINDOW_QUERIES, KEY_VALUE_HEADS, QUERY_PER_GROUP, HEAD_DIMENSION).transpose(1, 0, 2, 3).reshape(KEY_VALUE_HEADS, WINDOW_QUERIES * QUERY_PER_GROUP, HEAD_DIMENSION)
    positions = jnp.arange(PROMPT_TOKENS).astype(jnp.float32)
    tokidx = jnp.arange(PROMPT_TOKENS).astype(jnp.int32)
    reach = (KERNEL_LIMIT - 1) // 2

    def per_group(items):
        kraw, vraw, qrows, wlen, kwidth, keep = items
        keys = rotate(kraw, positions).astype(jnp.bfloat16)
        vmag = lax.optimization_barrier(jnp.mean(jnp.abs(vraw), axis=1))
        scores = lax.dot_general(qrows, keys, (((1,), (1,)), ((), ())), preferred_element_type=jnp.float32) * HEAD_DIMENSION ** (-0.5)
        limit = jnp.repeat(PROMPT_TOKENS - WINDOW_QUERIES + jnp.arange(WINDOW_QUERIES).astype(jnp.int32), QUERY_PER_GROUP)
        allowed = tokidx[None, :] <= limit[:, None]
        scores = jnp.where(allowed, scores, jnp.float32(-1e+30))
        top = lax.optimization_barrier(jnp.max(scores, axis=1))
        expo = jnp.exp(scores - top[:, None])
        total = lax.optimization_barrier(jnp.sum(expo, axis=1))
        used = (jnp.arange(WINDOW_QUERIES).astype(jnp.int32) >= WINDOW_QUERIES - wlen).astype(jnp.float32)
        rowwt = jnp.repeat(used, QUERY_PER_GROUP) / total
        column = jnp.dot(rowwt, expo, precision=lax.Precision.HIGHEST) * vmag
        padded = jnp.pad(column, reach)
        kernel_halfspan = (kwidth - 1) // 2
        pooled = column
        for shift in range(1, reach + 1):
            wider = jnp.maximum(jnp.maximum(pooled, padded[reach + shift:reach + shift + PROMPT_TOKENS]), padded[reach - shift:reach - shift + PROMPT_TOKENS])
            pooled = jnp.where(shift <= kernel_halfspan, wider, pooled)
        scored = lax.optimization_barrier(jnp.sum(pooled.reshape(KEY_BLOCK_COUNT, BLK), axis=1))
        ordered = -jnp.sort(-scored)
        ranks = jnp.arange(KEY_BLOCK_COUNT).astype(jnp.int32)
        kept = jnp.sum(jnp.where(ranks < keep, ordered, jnp.float32(0.0)))
        return (scored, kept / jnp.sum(scored))
    block_scores, kept_fraction = lax.map(per_group, (key_states_full, value_states_full, query_states_full, window_len, kernel_width, kept_block_count))
    return (block_scores, kept_fraction)
```

```python
import jax
import jax.numpy as jnp
from jax import lax
from jax.sharding import PartitionSpec as P

BLK = 128
KERNEL_LIMIT = 15
HALO = 8
CORES = 2
GROUP = 4


def rotary(head_size, positions):
    half = head_size // 2
    freq = 500000.0 ** (-(jnp.arange(half).astype(jnp.float32) * 2.0) / head_size)
    angle = positions[:, None] * freq[None, :]
    return jnp.cos(angle), jnp.sin(angle)


def local(
    hidden, gain, key_matrix, value_matrix, queries, window_len, kernel_width, kept_block_count
):
    tok_rows, feats = hidden.shape
    full_width = gain.shape[0]
    head_size = key_matrix.shape[1]
    n_seq, n_head = lax.axis_size("seq"), lax.axis_size("head")
    n_x = n_head // CORES
    s, h = lax.axis_index("seq"), lax.axis_index("head")
    x, c = h // CORES, h % CORES
    i = s % GROUP
    r = feats // 2
    total_tokens = tok_rows * n_seq

    def shift_x(offset):
        return [
            (a * CORES + b, (a + offset) % n_x * CORES + b) for a in range(n_x) for b in range(CORES)
        ]

    def flip(bit):
        return [(j, j ^ bit) for j in range(n_seq)]

    def rows_at(start, count):
        return jnp.concatenate(
            [
                lax.dynamic_slice_in_dim(key_matrix, start, count, axis=0),
                lax.dynamic_slice_in_dim(value_matrix, start, count, axis=0),
            ],
            axis=1,
        )

    def start_of(chip, j):
        return (chip * CORES + jnp.where(j >= 2, 1 - c, c)) * feats + (j % 2) * r

    crossing = []
    for o in range(1, n_x):
        chip = (x - o) % n_x
        first = lax.ppermute(rows_at(start_of(chip, i), r), "head", shift_x(-o))
        second = lax.ppermute(rows_at(start_of(chip, 3 - i), r), "head", shift_x(-o))
        by_y = lax.ppermute(first, "seq", flip(1))
        by_z = lax.ppermute(first, "seq", flip(2))
        crossing.append((first, by_y, by_z, second))

    before = lax.ppermute(hidden[tok_rows - HALO :], "seq", [(j, j + 1) for j in range(n_seq - 1)])
    after = lax.ppermute(hidden[:HALO], "seq", [(j + 1, j) for j in range(n_seq - 1)])
    mine = jnp.concatenate([before, hidden, after], axis=0)
    other = lax.ppermute(mine, "head", [(j, j ^ 1) for j in range(n_head)])

    mine_f, other_f = mine.astype(jnp.float32), other.astype(jnp.float32)
    sumsq = jnp.sum(mine_f * mine_f, axis=1) + jnp.sum(other_f * other_f, axis=1)
    total_sq = sumsq
    for o in range(1, n_x):
        total_sq = total_sq + lax.ppermute(sumsq, "head", shift_x(o))
    inv_rms = lax.rsqrt(total_sq / full_width + 1e-05)

    mine_at, other_at = h * feats, (h ^ 1) * feats
    mine_gain = lax.dynamic_slice_in_dim(gain, mine_at, feats)
    other_gain = lax.dynamic_slice_in_dim(gain, other_at, feats)
    normed = jnp.concatenate(
        [
            (mine_f * mine_gain[None, :]).astype(jnp.bfloat16),
            (other_f * other_gain[None, :]).astype(jnp.bfloat16),
        ],
        axis=1,
    )

    def dot(a, b):
        return jnp.dot(a, b, preferred_element_type=jnp.float32)

    projected = dot(normed[:, :feats], rows_at(mine_at, feats))
    projected = projected + dot(normed[:, feats:], rows_at(other_at, feats))
    slabs = [lax.dynamic_slice_in_dim(normed, (i ^ k) * r, r, axis=1) for k in range(GROUP)]
    for o in range(1, n_x):
        partial = sum(dot(a, b) for a, b in zip(slabs, crossing[o - 1]))
        projected = projected + lax.ppermute(
            partial.astype(jnp.bfloat16), "head", shift_x(o)
        ).astype(jnp.float32)

    projected = projected * inv_rms[:, None]
    span = tok_rows + 2 * HALO
    tok_index = s * tok_rows - HALO + jnp.arange(span)
    cos, sin = rotary(head_size, tok_index.astype(jnp.float32))
    half = head_size // 2
    lead, trail = projected[:, :half], projected[:, half:head_size]
    keys = jnp.concatenate([lead * cos - trail * sin, trail * cos + lead * sin], axis=1)
    keys = keys.astype(jnp.bfloat16)
    vmag = jnp.mean(jnp.abs(projected[:, head_size:]), axis=1)

    window = queries.shape[0]
    group_heads = queries.shape[1] // head_size
    query_rows = queries.reshape(window * group_heads, head_size)
    scores = lax.dot_general(
        keys, query_rows, (((1,), (1,)), ((), ())), preferred_element_type=jnp.float32
    ) * head_size ** (-0.5)
    row_window = jnp.arange(window * group_heads) // group_heads
    limit = total_tokens - window + row_window
    allowed = (tok_index[:, None] <= limit[None, :]) & (tok_index[:, None] >= 0)
    scores = jnp.where(allowed, scores, jnp.float32(-1e30))
    top = jnp.max(scores, axis=0)
    expo = jnp.exp(scores - top[None, :])
    own_total = jnp.sum(expo[HALO : HALO + tok_rows], axis=0)
    stats = jnp.broadcast_to(jnp.stack([top, own_total])[None], (n_seq, 2, top.shape[0]))
    stats = lax.all_to_all(stats, "seq", 0, 0, tiled=True)
    row_top = jnp.max(stats[:, 0], axis=0)
    row_total = jnp.sum(stats[:, 1] * jnp.exp(stats[:, 0] - row_top[None, :]), axis=0)
    used = (row_window >= window - window_len[0]).astype(jnp.float32)
    row_weight = used * jnp.exp(top - row_top) / row_total
    column = (
        lax.dot_general(
            row_weight[None, :], expo, (((1,), (1,)), ((), ())), precision=lax.Precision.HIGHEST
        )[0]
        * vmag
    )
    reach = (KERNEL_LIMIT - 1) // 2
    kernel_halfspan = (kernel_width[0] - 1) // 2
    pooled = column[HALO : HALO + tok_rows]
    for shift in range(1, reach + 1):
        wider = jnp.maximum(
            jnp.maximum(pooled, column[HALO + shift : HALO + shift + tok_rows]),
            column[HALO - shift : HALO - shift + tok_rows],
        )
        pooled = jnp.where(shift <= kernel_halfspan, wider, pooled)
    local_blocks = jnp.sum(pooled.reshape(tok_rows // BLK, BLK), axis=1)[None, :]
    spread = jnp.broadcast_to(local_blocks, (n_seq, local_blocks.shape[1]))
    everything = lax.all_to_all(spread, "seq", 0, 0, tiled=True).reshape(-1)
    ordered = -jnp.sort(-everything)
    ranks = jnp.arange(ordered.shape[0])
    kept = jnp.sum(jnp.where(ranks < kept_block_count[0], ordered, jnp.float32(0.0)))
    fraction = (kept / jnp.sum(ordered)).reshape(1)
    return (local_blocks, fraction)


def solution(mesh):
    return jax.shard_map(
        local,
        mesh=mesh,
        in_specs=(
            P("seq", "head"),
            P(),
            P(None, "head"),
            P(None, "head"),
            P(None, "head"),
            P("head"),
            P("head"),
            P("head"),
        ),
        out_specs=(P("head", "seq"), P("head")),
        check_vma=False,
    )
```

```python
import functools

import jax
import jax.numpy as jnp
from jax import lax
from jax.experimental import pallas as pl
from jax.experimental.pallas import tpu as pltpu
from jax.sharding import PartitionSpec as P

BLK = 128
LANES = 128
KERNEL_LIMIT = 15
HALO = 8
CORES = 2
GROUP = 4
MASKED = -1e30

VMEM = pl.BlockSpec(memory_space=pltpu.VMEM)
SMEM = pl.BlockSpec(memory_space=pltpu.SMEM)
HBM = pl.BlockSpec(memory_space=pltpu.HBM)
F32, BF16 = jnp.float32, jnp.bfloat16


def sds(shape, dtype):
    return jax.ShapeDtypeStruct(shape, dtype)


def call(body, out, ins, scratch=(), outs=None, flops=1 << 20, limit=40 << 20):
    return pl.pallas_call(
        body,
        out_shape=out,
        in_specs=ins,
        out_specs=outs if outs is not None else jax.tree.map(lambda _: VMEM, out),
        scratch_shapes=list(scratch),
        cost_estimate=pl.CostEstimate(flops=flops, bytes_accessed=1 << 20, transcendentals=0),
        compiler_params=pltpu.CompilerParams(vmem_limit_bytes=limit),
    )


def iota(shape, dim):
    return lax.broadcasted_iota(jnp.int32, shape, dim)


def to_lanes(col):
    n = col.shape[0]
    here = iota((n, LANES), 0) == iota((n, LANES), 1)
    return jnp.sum(jnp.where(here, jnp.broadcast_to(col, (n, LANES)), 0.0), axis=0, keepdims=True)


def to_rows(row, n):
    here = iota((n, LANES), 0) == iota((n, LANES), 1)
    return jnp.sum(jnp.where(here, jnp.broadcast_to(row, (n, LANES)), 0.0), axis=1, keepdims=True)


def pack_kernel(chunks, at, km, vm, *refs):
    outs, sem = refs[:-1], refs[-1]
    head = km.shape[1]
    copies = []
    for which, (out_no, to, count) in enumerate(chunks):
        start = pl.multiple_of(at[which], 128)
        for side, src in enumerate((km, vm)):
            copies.append(
                pltpu.make_async_copy(
                    src.at[pl.ds(start, count)],
                    outs[out_no].at[pl.ds(to, count), pl.ds(side * head, head)],
                    sem.at[2 * which + side],
                )
            )
    for c in copies:
        c.start()
    for c in copies:
        c.wait()


def norm_kernel(
    at, hid, swp, halo, swp_halo, gain, km, vm, normed, sumsq, acc_k, acc_v, wbuf, total, sem
):
    tok, feats = hid.shape
    head = km.shape[1]
    copies = []
    for part in range(CORES):
        start = pl.multiple_of(at[part], 128)
        for side, src in enumerate((km, vm)):
            copies.append(
                pltpu.make_async_copy(
                    src.at[pl.ds(start, feats)],
                    wbuf.at[pl.ds(part * feats, feats), pl.ds(side * head, head)],
                    sem.at[2 * part + side],
                )
            )
    for c in copies:
        c.start()
    sumsq[...] = jnp.zeros_like(sumsq)
    pieces = [(b * LANES, LANES, b) for b in range(tok // LANES)] + [(tok, 2 * HALO, tok // LANES)]
    for row, count, line in pieces:
        folded = jnp.zeros((count, LANES), F32)
        for part, (main, edge) in enumerate(((hid, halo), (swp, swp_halo))):
            for t in range(feats // LANES):
                lanes = pl.ds(t * LANES, LANES)
                raw = (main[pl.ds(row, count), lanes] if row < tok else edge[:, lanes]).astype(F32)
                folded = folded + raw * raw
                g = gain[pl.ds(part, 1), lanes]
                normed[pl.ds(row, count), pl.ds(part * feats + t * LANES, LANES)] = (raw * g).astype(BF16)
        sumsq[pl.ds(line, 1), :] = to_lanes(jnp.sum(folded, axis=1, keepdims=True))
    for c in copies:
        c.wait()
    total[...] = jnp.zeros_like(total)
    step = min(1024, feats)

    def body(k, carry):
        at_k = pl.multiple_of(k * step, 128)
        total[...] += jnp.dot(
            normed[:, pl.ds(at_k, step)], wbuf[pl.ds(at_k, step), :], preferred_element_type=F32
        )
        return carry

    lax.fori_loop(0, CORES * feats // step, body, 0)
    acc_k[...] = total[:, :head]
    acc_v[...] = total[:, head:]


def partial_kernel(r, hw, at, normed, b0, b1, b2, b3, out_k, out_v):
    head = out_k.shape[1]
    total = None
    for k, blk in enumerate((b0, b1, b2, b3)):
        col = pl.multiple_of(at[k], 128)
        p = jnp.dot(normed[:, pl.ds(col, r)], blk[:r, :], preferred_element_type=F32)
        total = p if total is None else total + p
    d2 = hw - 2 * r
    if d2:
        for part in range(CORES):
            total = total + jnp.dot(
                normed[:, pl.ds(part * hw + 2 * r, d2)],
                b3[r + part * d2 : r + (part + 1) * d2, :],
                preferred_element_type=F32,
            )
    out_k[...] = total[:, :head].astype(BF16)
    out_v[...] = total[:, head:].astype(BF16)


def row_scale(sumsq, tok, full_width):
    inv = lax.rsqrt(sumsq / full_width + 1e-05)
    parts = [to_rows(inv[b : b + 1, :], LANES) for b in range(tok // LANES)]
    parts.append(to_rows(inv[tok // LANES : tok // LANES + 1, :], 2 * HALO))
    return parts


def score_kernel(full_width, scale_by, first, *refs):
    n_off = (len(refs) - 9) // 2
    acc, parts, sqs = refs[0], refs[1 : 1 + n_off], refs[1 + n_off : 2 + 2 * n_off]
    cos, sin, q, limit, expo, stats, keys = refs[2 + 2 * n_off :]
    span, head = acc.shape
    tok = span - 2 * HALO
    sumsq = sqs[0][...]
    for sq in sqs[1:]:
        sumsq = sumsq + sq[...]
    row = 0
    for col in row_scale(sumsq, tok, full_width):
        n = col.shape[0]
        k = acc[row : row + n, :]
        for p in parts:
            k = k + p[row : row + n, :].astype(F32)
        k = k * col
        rot = k * cos[row : row + n, :] + pltpu.roll(k, head // 2, 1) * sin[row : row + n, :]
        keys[row : row + n, :] = rot.astype(BF16)
        row += n
    scores = lax.dot_general(
        keys[...], q[...], (((1,), (1,)), ((), ())), preferred_element_type=F32
    ) * scale_by
    idx = iota((span, 1), 0)
    token = jnp.where(idx < tok, first[0] + idx, jnp.where(idx < tok + HALO, first[0] - HALO + idx - tok, first[0] + idx - HALO))
    token = jnp.where(token < 0, jnp.int32(2**30), token)
    scores = jnp.where(token <= limit[...], scores, MASKED)
    top = jnp.max(scores, axis=0, keepdims=True)
    e = jnp.exp(scores - top)
    expo[...] = e
    own = jnp.sum(e[:tok, :], axis=0, keepdims=True)
    for d in range(stats.shape[0]):
        stats[d, 0:1, :] = top
        stats[d, 1:2, :] = own


def pool_kernel(full_width, window, sizes, got, mine, expo, *refs):
    n_off = (len(refs) - 5) // 2
    acc, parts, sqs = refs[0], refs[1 : 1 + n_off], refs[1 + n_off : 2 + 2 * n_off]
    win, blocks, spread = refs[2 + 2 * n_off :]
    span = expo.shape[0]
    tok = span - 2 * HALO
    nb = tok // LANES
    row_top = got[0, 0:1, :]
    for d in range(1, got.shape[0]):
        row_top = jnp.maximum(row_top, got[d, 0:1, :])
    row_total = jnp.zeros_like(row_top)
    for d in range(got.shape[0]):
        row_total = row_total + got[d, 1:2, :] * jnp.exp(got[d, 0:1, :] - row_top)
    weight = jnp.exp(mine[0, 0:1, :] - row_top) / row_total
    weight = jnp.where(win[...] >= window - sizes[0], weight, 0.0)
    sumsq = sqs[0][...]
    for sq in sqs[1:]:
        sumsq = sumsq + sq[...]
    scales = row_scale(sumsq, tok, full_width)
    lines = []
    row = 0
    for col in scales:
        n = col.shape[0]
        v = acc[row : row + n, :]
        for p in parts:
            v = v + p[row : row + n, :].astype(F32)
        vmag = jnp.sum(jnp.abs(v), axis=1, keepdims=True) * (1.0 / v.shape[1]) * col
        mass = jnp.sum(expo[row : row + n, :] * weight, axis=1, keepdims=True)
        lines.append(to_lanes(mass * vmag))
        row += n
    edge = pltpu.roll(lines[nb], LANES - HALO, 1)
    height = -(-(nb + 2) // 8) * 8
    line = iota((height, LANES), 0)
    lane = iota((height, LANES), 1)
    column = jnp.broadcast_to(edge, (height, LANES))
    for b in range(nb):
        column = jnp.where(line == b, jnp.broadcast_to(lines[b], (height, LANES)), column)
    below, above = pltpu.roll(column, height - 1, 0), pltpu.roll(column, 1, 0)
    halfspan = lax.shift_right_arithmetic(sizes[1] - 1, 1)
    pooled = column
    for shift in range(1, (KERNEL_LIMIT - 1) // 2 + 1):
        right = pltpu.roll(jnp.where(lane < shift, below, column), LANES - shift, 1)
        left = pltpu.roll(jnp.where(lane >= LANES - shift, above, column), shift, 1)
        wider = jnp.maximum(jnp.maximum(pooled, right), left)
        pooled = jnp.where(shift <= halfspan, wider, pooled)
    sums = jnp.sum(pooled, axis=1, keepdims=True)
    pick = (line == lax.rem(lane, nb)) & (line < nb)
    flat = jnp.sum(jnp.where(pick, jnp.broadcast_to(sums, (height, LANES)), 0.0), axis=0, keepdims=True)
    blocks[...] = flat[:, :nb]
    spread[...] = jnp.broadcast_to(flat, spread.shape)


def rank_kernel(nb, keep, everything, out):
    v = everything[...]
    n = v.shape[0]
    place = iota(v.shape, 0) * nb + lax.rem(iota(v.shape, 1), nb)
    rank = jnp.zeros(v.shape, jnp.int32)
    for a in range(nb):
        va = pltpu.roll(v, a, 1) if a else v
        pa = pltpu.roll(place, a, 1) if a else place
        for b in range(n):
            vb = pltpu.roll(va, b, 0) if b else va
            pb = pltpu.roll(pa, b, 0) if b else pa
            rank = rank + jnp.where((vb > v) | ((vb == v) & (pb < place)), 1, 0)
    once = iota(v.shape, 1) < nb
    kept = jnp.where(once & (rank < keep[0]), v, 0.0)
    whole = jnp.where(once, v, 0.0)

    def add(t):
        return jnp.sum(jnp.sum(t, axis=1, keepdims=True), axis=0, keepdims=True)

    out[...] = add(kept) / add(whole)


def local(
    hidden, gain, key_matrix, value_matrix, queries, window_len, kernel_width, kept_block_count
):
    tok, feats = hidden.shape
    full_width = gain.shape[0]
    head = key_matrix.shape[1]
    n_seq, n_head = lax.axis_size("seq"), lax.axis_size("head")
    n_x = n_head // CORES
    s, h = lax.axis_index("seq"), lax.axis_index("head")
    x, c = h // CORES, h % CORES
    i = s % GROUP
    r = feats * 7 // 16 // LANES * LANES
    spare = feats - 2 * r
    span = tok + 2 * HALO
    total_tokens = tok * n_seq

    def shift_x(offset):
        return [
            (a * CORES + b, (a + offset) % n_x * CORES + b) for a in range(n_x) for b in range(CORES)
        ]

    def flip(bit):
        return [(j, j ^ bit) for j in range(n_seq)]

    def half_at(chip, part):
        return (chip * CORES + jnp.where(part == 0, c, 1 - c)) * feats

    def block_at(chip, j):
        return half_at(chip, j // 2) + (j % 2) * r

    offsets = range(1, n_x)
    starts, chunks = [], []
    for o in offsets:
        chip = (x - o) % n_x
        starts += [block_at(chip, i), block_at(chip, 3 - i)]
        starts += [half_at(chip, part) + 2 * r for part in range(CORES)]
        a = 2 * (o - 1)
        chunks += [(a, 0, r), (a + 1, 0, r), (a + 1, r, spare), (a + 1, r + spare, spare)]
    rows = [r, r + CORES * spare] * len(offsets)
    packed = call(
        functools.partial(pack_kernel, tuple(chunks)),
        [sds((n, 2 * head), BF16) for n in rows],
        [SMEM, HBM, HBM],
        scratch=[pltpu.SemaphoreType.DMA((2 * len(chunks),))],
        limit=8 << 20,
    )(jnp.stack(starts), key_matrix, value_matrix)

    firsts, seconds = [], []
    for o in offsets:
        firsts.append(lax.ppermute(packed[2 * o - 2], "head", shift_x(-o)))
        seconds.append(lax.ppermute(packed[2 * o - 1], "head", shift_x(-o)))
    swapped = lax.ppermute(hidden, "head", [(j, j ^ 1) for j in range(n_head)])
    before = lax.ppermute(hidden[tok - HALO :], "seq", [(j, j + 1) for j in range(n_seq - 1)])
    after = lax.ppermute(hidden[:HALO], "seq", [(j + 1, j) for j in range(n_seq - 1)])
    halo = jnp.concatenate([before, after], axis=0)
    swapped_halo = lax.ppermute(halo, "head", [(j, j ^ 1) for j in range(n_head)])
    crossing = []
    for o in offsets:
        by_y = lax.ppermute(firsts[o - 1], "seq", flip(1))
        by_z = lax.ppermute(firsts[o - 1], "seq", flip(2))
        crossing.append((firsts[o - 1], by_y, by_z, seconds[o - 1]))

    gains = jnp.stack(
        [lax.dynamic_slice_in_dim(gain, p * feats, feats) for p in (h, h ^ 1)], axis=0
    )
    lines = -(-(tok // LANES + 1) // 8) * 8
    normed, sumsq, acc_k, acc_v = call(
        norm_kernel,
        [
            sds((span, CORES * feats), BF16),
            sds((lines, LANES), F32),
            sds((span, head), F32),
            sds((span, head), F32),
        ],
        [SMEM, VMEM, VMEM, VMEM, VMEM, VMEM, HBM, HBM],
        scratch=[
            pltpu.VMEM((CORES * feats, 2 * head), BF16),
            pltpu.VMEM((span, 2 * head), F32),
            pltpu.SemaphoreType.DMA((2 * CORES,)),
        ],
        flops=1 << 31,
    )(
        jnp.stack([h * feats, (h ^ 1) * feats]),
        hidden, swapped, halo, swapped_halo, gains, key_matrix, value_matrix,
    )
    sqs = [sumsq] + [lax.ppermute(sumsq, "head", shift_x(o)) for o in offsets]

    parts_k, parts_v = [], []
    slabs = jnp.stack([((i ^ k) // 2) * feats + ((i ^ k) % 2) * r for k in range(GROUP)])
    for o in offsets:
        part_k, part_v = call(
            functools.partial(partial_kernel, r, feats),
            [sds((span, head), BF16), sds((span, head), BF16)],
            [SMEM] + [VMEM] * 5,
            flops=1 << 31,
        )(slabs, normed, *crossing[o - 1])
        parts_k.append(lax.ppermute(part_k, "head", shift_x(o)))
        parts_v.append(lax.ppermute(part_v, "head", shift_x(o)))

    half = head // 2
    freq = 500000.0 ** (-(jnp.arange(half).astype(F32) * 2.0) / head)
    at = jnp.arange(span)
    token = s * tok + jnp.where(
        at < tok, at, jnp.where(at < tok + HALO, at - tok - HALO, at - HALO)
    )
    angle = token.astype(F32)[:, None] * freq[None, :]
    cos, sin = jnp.cos(angle), jnp.sin(angle)
    cos = jnp.concatenate([cos, cos], axis=1)
    sin = jnp.concatenate([-sin, sin], axis=1)

    window = queries.shape[0]
    group_heads = queries.shape[1] // head
    rows = window * group_heads
    query_rows = queries.reshape(rows, head)
    row_window = (jnp.arange(rows) // group_heads).astype(jnp.int32)[None, :]
    limit = total_tokens - window + row_window
    expo, stats = call(
        functools.partial(score_kernel, full_width, head ** (-0.5)),
        [sds((span, rows), F32), sds((n_seq, 2, rows), F32)],
        [SMEM] + [VMEM] * (6 + 2 * len(offsets)),
        scratch=[pltpu.VMEM((span, head), BF16)],
        flops=1 << 28,
    )((s * tok).reshape(1), acc_k, *parts_k, *sqs, cos, sin, query_rows, limit)
    got = lax.all_to_all(stats, "seq", 0, 0, tiled=True)
    nb = tok // BLK
    local_blocks, spread = call(
        functools.partial(pool_kernel, full_width, window),
        [sds((1, nb), F32), sds((n_seq, LANES), F32)],
        [SMEM] + [VMEM] * (6 + 2 * len(offsets)),
        flops=1 << 26,
    )(
        jnp.concatenate([window_len, kernel_width]),
        got, stats, expo, acc_v, *parts_v, *sqs, row_window,
    )
    everything = lax.all_to_all(spread, "seq", 0, 0, tiled=True)
    fraction = call(
        functools.partial(rank_kernel, nb), sds((1, 1), F32), [SMEM, VMEM], flops=1 << 20
    )(kept_block_count, everything)
    return (local_blocks, fraction.reshape(1))


def solution(mesh):
    return jax.shard_map(
        local,
        mesh=mesh,
        in_specs=(
            P("seq", "head"),
            P(),
            P(None, "head"),
            P(None, "head"),
            P(None, "head"),
            P("head"),
            P("head"),
            P("head"),
        ),
        out_specs=(P("head", "seq"), P("head")),
        check_vma=False,
    )
```

```python
import functools

import jax
import jax.numpy as jnp
from jax import lax
from jax.experimental import pallas as pl
from jax.experimental.pallas import tpu as pltpu
from jax.sharding import PartitionSpec as P

BLK = 128
LANES = 128
KERNEL_LIMIT = 15
REACH = (KERNEL_LIMIT - 1) // 2
EDGE = 16
CORES = 2
GROUP = 4
MASKED = -1e30

VMEM = pl.BlockSpec(memory_space=pltpu.VMEM)
SMEM = pl.BlockSpec(memory_space=pltpu.SMEM)
HBM = pl.BlockSpec(memory_space=pltpu.HBM)
F32, BF16 = jnp.float32, jnp.bfloat16


def sds(shape, dtype):
    return jax.ShapeDtypeStruct(shape, dtype)


def call(body, out, ins, scratch=(), outs=None, flops=1 << 20, limit=40 << 20):
    return pl.pallas_call(
        body,
        out_shape=out,
        in_specs=ins,
        out_specs=outs if outs is not None else jax.tree.map(lambda _: VMEM, out),
        scratch_shapes=list(scratch),
        cost_estimate=pl.CostEstimate(flops=flops, bytes_accessed=1 << 20, transcendentals=0),
        compiler_params=pltpu.CompilerParams(vmem_limit_bytes=limit),
    )


def iota(shape, dim):
    return lax.broadcasted_iota(jnp.int32, shape, dim)


def to_lanes(col):
    n = col.shape[0]
    here = iota((n, LANES), 0) == iota((n, LANES), 1)
    return jnp.sum(jnp.where(here, jnp.broadcast_to(col, (n, LANES)), 0.0), axis=0, keepdims=True)


def to_rows(row, n):
    here = iota((n, LANES), 0) == iota((n, LANES), 1)
    return jnp.sum(jnp.where(here, jnp.broadcast_to(row, (n, LANES)), 0.0), axis=1, keepdims=True)


def pack_kernel(chunks, at, km, vm, out, sem):
    head = km.shape[1]
    copies = []
    for which, (to, count) in enumerate(chunks):
        start = pl.multiple_of(at[which], LANES)
        for side, src in enumerate((km, vm)):
            copies.append(
                pltpu.make_async_copy(
                    src.at[pl.ds(start, count)],
                    out.at[pl.ds(to, count), pl.ds(side * head, head)],
                    sem.at[2 * which + side],
                )
            )
    for c in copies:
        c.start()
    for c in copies:
        c.wait()


def norm_kernel(at, hid, gain, weights, *refs):
    more = refs[:-3]
    normed, sumsq, acc = refs[-3:]
    tok, feats = hid.shape
    line = at[0] // LANES
    nb = tok // LANES
    sumsq[...] = more[0][...] if more else jnp.zeros_like(sumsq)
    for b in range(nb):
        rows = pl.ds(b * LANES, LANES)
        folded = None
        for t in range(feats // LANES):
            lanes = pl.ds(t * LANES, LANES)
            raw = hid[rows, lanes].astype(F32)
            folded = raw * raw if folded is None else folded + raw * raw
            normed[rows, lanes] = (raw * gain[pl.ds(line + t, 1), :]).astype(BF16)
        sumsq[b : b + 1, :] += to_lanes(jnp.sum(folded, axis=1, keepdims=True))
    out = jnp.dot(normed[...], weights[...], preferred_element_type=F32)
    acc[...] = out + more[1][...] if more else out


def part_of(q, at, mine, other, blk):
    a = mine[:, pl.ds(pl.multiple_of(at * q[0], LANES), q[0])]
    b = other[:, pl.ds(pl.multiple_of(at * q[1], LANES), q[1])]
    return jnp.dot(a, blk[: q[0], :], preferred_element_type=F32) + jnp.dot(
        b, blk[q[0] : q[0] + q[1], :], preferred_element_type=F32
    )


def early_kernel(q, at, mine, other, b0, out):
    out[...] = part_of(q, at[0], mine, other, b0)


def late_kernel(q, at, mine, other, early, b1, b2, b3, out_k, out_v):
    head = out_k.shape[1]
    total = early[...]
    for k, blk in enumerate((b1, b2, b3)):
        total = total + part_of(q, at[k + 1], mine, other, blk)
    total = total + jnp.dot(
        other[:, GROUP * q[1] :], b3[q[0] + q[1] :, :], preferred_element_type=F32
    )
    out_k[...] = total[:, :head].astype(BF16)
    out_v[...] = total[:, head:].astype(BF16)


def row_scale(sqs, tok, full_width):
    sumsq = sqs[0][...]
    for sq in sqs[1:]:
        sumsq = sumsq + sq[...]
    inv = lax.rsqrt(sumsq / full_width + 1e-05)
    return [to_rows(inv[b : b + 1, :], LANES) for b in range(tok // LANES)]


def score_kernel(full_width, scale_by, first, *refs):
    n_off = (len(refs) - 9) // 2
    acc, parts, sqs = refs[0], refs[1 : 1 + n_off], refs[1 + n_off : 2 + 2 * n_off]
    cos, sin, q, limit, expo, stats, keys = refs[2 + 2 * n_off :]
    tok, head = keys.shape
    for b, col in enumerate(row_scale(sqs, tok, full_width)):
        rows = pl.ds(b * LANES, LANES)
        k = acc[rows, :head]
        for p in parts:
            k = k + p[rows, :].astype(F32)
        k = k * col
        keys[rows, :] = (k * cos[rows, :] + pltpu.roll(k, head // 2, 1) * sin[rows, :]).astype(BF16)
    scores = lax.dot_general(
        keys[...], q[...], (((1,), (1,)), ((), ())), preferred_element_type=F32
    ) * scale_by
    token = first[0] + iota((tok, 1), 0)
    scores = jnp.where(token <= limit[...], scores, MASKED)
    top = jnp.max(scores, axis=0, keepdims=True)
    e = jnp.exp(scores - top)
    expo[...] = e
    own = jnp.sum(e, axis=0, keepdims=True)
    for d in range(stats.shape[0]):
        stats[d, 0:1, :] = top
        stats[d, 1:2, :] = own


def widen(column, below, above, lane, halfspan):
    pooled = column
    for shift in range(1, REACH + 1):
        right = pltpu.roll(jnp.where(lane < shift, below, column), LANES - shift, 1)
        left = pltpu.roll(jnp.where(lane >= LANES - shift, above, column), shift, 1)
        pooled = jnp.where(
            shift <= halfspan, jnp.maximum(jnp.maximum(pooled, right), left), pooled
        )
    return pooled


def pool_kernel(full_width, window, sizes, got, mine, expo, *refs):
    n_off = (len(refs) - 4) // 2
    acc, parts, sqs = refs[0], refs[1 : 1 + n_off], refs[1 + n_off : 2 + 2 * n_off]
    win, spread = refs[2 + 2 * n_off :]
    tok = expo.shape[0]
    head = acc.shape[1] // 2
    nb = tok // LANES
    row_top = got[0, 0:1, :]
    for d in range(1, got.shape[0]):
        row_top = jnp.maximum(row_top, got[d, 0:1, :])
    row_total = jnp.zeros_like(row_top)
    for d in range(got.shape[0]):
        row_total = row_total + got[d, 1:2, :] * jnp.exp(got[d, 0:1, :] - row_top)
    weight = jnp.exp(mine[0, 0:1, :] - row_top) / row_total
    weight = jnp.where(win[...] >= window - sizes[0], weight, 0.0)
    height = -(-nb // 8) * 8
    line = iota((height, LANES), 0)
    lane = iota((height, LANES), 1)
    column = jnp.zeros((height, LANES), F32)
    for b, col in enumerate(row_scale(sqs, tok, full_width)):
        rows = pl.ds(b * LANES, LANES)
        v = acc[rows, head:]
        for p in parts:
            v = v + p[rows, :].astype(F32)
        vmag = jnp.sum(jnp.abs(v), axis=1, keepdims=True) * (1.0 / head) * col
        mass = jnp.sum(expo[rows, :] * weight, axis=1, keepdims=True)
        here = jnp.broadcast_to(to_lanes(mass * vmag), (height, LANES))
        column = jnp.where(line == b, here, column)
    below, above = pltpu.roll(column, height - 1, 0), pltpu.roll(column, 1, 0)
    halfspan = lax.shift_right_arithmetic(sizes[1] - 1, 1)
    pooled = widen(column, below, above, lane, halfspan)
    place = line * LANES + lane
    inner = (place >= REACH) & (place < tok - REACH)
    sums = to_lanes(jnp.sum(jnp.where(inner, pooled, 0.0), axis=1, keepdims=True))
    flat = lane[0:1, :]
    last = pltpu.roll(column[nb - 1 : nb, :], 2 * EDGE, 1)
    said = jnp.where(flat < EDGE, column[0:1, :], jnp.where(flat < 2 * EDGE, last, pltpu.roll(sums, 2 * EDGE, 1)))
    spread[...] = jnp.broadcast_to(said, spread.shape)


def rank_kernel(nb, sizes, said, blocks, share):
    v = said[...]
    n = v.shape[0]
    line, lane = iota(v.shape, 0), iota(v.shape, 1)
    following = pltpu.roll(v, n - 1, 0)
    seam = jnp.where(lane < EDGE, pltpu.roll(v, LANES - EDGE, 1), pltpu.roll(following, EDGE, 1))
    seam = jnp.where(lane < 2 * EDGE, seam, 0.0)
    end = line == n - 1
    zero = jnp.zeros_like(seam)
    halfspan = lax.shift_right_arithmetic(sizes[1] - 1, 1)
    tail = widen(jnp.where(end & (lane >= EDGE), 0.0, seam), zero, zero, lane, halfspan)
    lead = widen(jnp.where(end & (lane < EDGE), 0.0, seam), zero, zero, lane, halfspan)
    tail = jnp.sum(jnp.where((lane >= EDGE - REACH) & (lane < EDGE), tail, 0.0), axis=1, keepdims=True)
    lead = jnp.sum(jnp.where((lane >= EDGE) & (lane < EDGE + REACH), lead, 0.0), axis=1, keepdims=True)
    lead = pltpu.roll(jnp.broadcast_to(lead, v.shape), 1, 0)
    b = pltpu.roll(v, LANES - 2 * EDGE, 1)
    b = b + jnp.where(lane == 0, lead, 0.0) + jnp.where(lane == nb - 1, tail, 0.0)
    b = jnp.where(lane < nb, b, 0.0)
    own = jnp.sum(jnp.where(line == sizes[2], b, 0.0), axis=0, keepdims=True)
    blocks[...] = own[:, :nb]
    place = line * nb + lane
    rank = jnp.zeros(v.shape, jnp.int32)

    def turned(t, k):
        return jnp.where(lane >= k, pltpu.roll(t, k, 1), pltpu.roll(t, LANES + k - nb, 1)) if k else t

    for k in range(nb):
        bk, pk = turned(b, k), turned(place, k)
        for m in range(n):
            bm, pm = (pltpu.roll(bk, m, 0), pltpu.roll(pk, m, 0)) if m else (bk, pk)
            rank = rank + jnp.where((bm > b) | ((bm == b) & (pm < place)), 1, 0)

    def add(t):
        return jnp.sum(jnp.sum(t, axis=1, keepdims=True), axis=0, keepdims=True)

    kept = jnp.where((lane < nb) & (rank < sizes[0]), b, 0.0)
    share[...] = add(kept) / add(b)


def local(
    hidden, gain, key_matrix, value_matrix, queries, window_len, kernel_width, kept_block_count
):
    tok, feats = hidden.shape
    full_width = gain.shape[0]
    head = key_matrix.shape[1]
    n_seq, n_head = lax.axis_size("seq"), lax.axis_size("head")
    n_x = n_head // CORES
    s, h = lax.axis_index("seq"), lax.axis_index("head")
    x, c = h // CORES, h % CORES
    i = s % GROUP
    q = (feats // GROUP, feats // GROUP - LANES)
    spare = feats - GROUP * q[1]
    total_tokens = tok * n_seq
    offsets = range(1, n_x)

    def shift_x(offset):
        return [
            (a * CORES + b, (a + offset) % n_x * CORES + b) for a in range(n_x) for b in range(CORES)
        ]

    def flip(bit):
        return [(j, j ^ bit) for j in range(n_seq)]

    def pack(starts, counts):
        to = [sum(counts[:k]) for k in range(len(counts))]
        return call(
            functools.partial(pack_kernel, tuple(zip(to, counts))),
            sds((sum(counts), 2 * head), BF16),
            [SMEM, HBM, HBM],
            scratch=[pltpu.SemaphoreType.DMA((2 * len(counts),))],
            limit=62 << 20,
        )(jnp.stack(starts), key_matrix, value_matrix)

    firsts, seconds = [], []
    for o in offsets:
        chip = (x - o) % n_x
        at0, at1 = (chip * CORES + c) * feats, (chip * CORES + 1 - c) * feats
        first = pack([at0 + i * q[0], at1 + i * q[1]], [q[0], q[1]])
        firsts.append(lax.ppermute(first, "head", shift_x(-o)))
        second = pack(
            [at0 + (3 - i) * q[0], at1 + (3 - i) * q[1], at1 + GROUP * q[1]], [q[0], q[1], spare]
        )
        seconds.append(lax.ppermute(second, "head", shift_x(-o)))
    swapped = lax.ppermute(hidden, "head", [(j, j ^ 1) for j in range(n_head)])
    trades = [[lax.ppermute(firsts[o - 1], "seq", flip(bit)) for bit in (1, 2)] for o in offsets]

    lines = -(-(tok // LANES) // 8) * 8
    gain_lines = gain.reshape(full_width // LANES, LANES)

    def norm(start, rows, more):
        weights = pack([start], [feats])
        return call(
            norm_kernel,
            [sds((tok, feats), BF16), sds((lines, LANES), F32), sds((tok, 2 * head), F32)],
            [SMEM] + [VMEM] * (3 + len(more)),
            flops=1 << 30,
        )(start.reshape(1), rows, gain_lines, weights, *more)

    mine, sumsq, acc = norm(h * feats, hidden, ())
    other, sumsq, acc = norm((h ^ 1) * feats, swapped, (sumsq, acc))
    sqs = [sumsq] + [lax.ppermute(sumsq, "head", shift_x(o)) for o in offsets]

    parts_k, parts_v = [], []
    slabs = jnp.stack([i ^ k for k in range(GROUP)])
    for o in offsets:
        early = call(
            functools.partial(early_kernel, q),
            sds((tok, 2 * head), F32),
            [SMEM] + [VMEM] * 3,
            flops=1 << 29,
        )(slabs, mine, other, firsts[o - 1])
        part_k, part_v = call(
            functools.partial(late_kernel, q),
            [sds((tok, head), BF16), sds((tok, head), BF16)],
            [SMEM] + [VMEM] * 6,
            flops=1 << 30,
        )(slabs, mine, other, early, *trades[o - 1], seconds[o - 1])
        parts_k.append(lax.ppermute(part_k, "head", shift_x(o)))
        parts_v.append(lax.ppermute(part_v, "head", shift_x(o)))

    half = head // 2
    freq = 500000.0 ** (-(jnp.arange(half).astype(F32) * 2.0) / head)
    token = s * tok + jnp.arange(tok)
    angle = token.astype(F32)[:, None] * freq[None, :]
    cos, sin = jnp.cos(angle), jnp.sin(angle)
    cos = jnp.concatenate([cos, cos], axis=1)
    sin = jnp.concatenate([-sin, sin], axis=1)

    window = queries.shape[0]
    group_heads = queries.shape[1] // head
    rows = window * group_heads
    query_rows = queries.reshape(rows, head)
    row_window = (jnp.arange(rows) // group_heads).astype(jnp.int32)[None, :]
    limit = total_tokens - window + row_window
    expo, stats = call(
        functools.partial(score_kernel, full_width, head ** (-0.5)),
        [sds((tok, rows), F32), sds((n_seq, 2, rows), F32)],
        [SMEM] + [VMEM] * (6 + 2 * len(offsets)),
        scratch=[pltpu.VMEM((tok, head), BF16)],
        flops=1 << 28,
    )((s * tok).reshape(1), acc, *parts_k, *sqs, cos, sin, query_rows, limit)
    got = lax.all_to_all(stats, "seq", 0, 0, tiled=True)
    nb = tok // BLK
    spread = call(
        functools.partial(pool_kernel, full_width, window),
        sds((n_seq, LANES), F32),
        [SMEM] + [VMEM] * (6 + 2 * len(offsets)),
        flops=1 << 26,
    )(
        jnp.concatenate([window_len, kernel_width]),
        got, stats, expo, acc, *parts_v, *sqs, row_window,
    )
    said = lax.all_to_all(spread, "seq", 0, 0, tiled=True)
    local_blocks, fraction = call(
        functools.partial(rank_kernel, nb),
        [sds((1, nb), F32), sds((1, 1), F32)],
        [SMEM, VMEM],
        flops=1 << 20,
    )(jnp.concatenate([kept_block_count, kernel_width, s.reshape(1)]), said)
    return (local_blocks, fraction.reshape(1))


def solution(mesh):
    return jax.shard_map(
        local,
        mesh=mesh,
        in_specs=(
            P("seq", "head"),
            P(),
            P(None, "head"),
            P(None, "head"),
            P(None, "head"),
            P("head"),
            P("head"),
            P("head"),
        ),
        out_specs=(P("head", "seq"), P("head")),
        check_vma=False,
    )
```

```python
import functools

import jax
import jax.numpy as jnp
from jax import lax
from jax.experimental import pallas as pl
from jax.experimental.pallas import tpu as pltpu
from jax.sharding import PartitionSpec as P

BLK = 128
LANES = 128
KERNEL_LIMIT = 15
REACH = (KERNEL_LIMIT - 1) // 2
EDGE = 16
CORES = 2
GROUP = 4
MASKED = -1e30

VMEM = pl.BlockSpec(memory_space=pltpu.VMEM)
SMEM = pl.BlockSpec(memory_space=pltpu.SMEM)
F32, BF16 = jnp.float32, jnp.bfloat16


def sds(shape, dtype):
    return jax.ShapeDtypeStruct(shape, dtype)


def call(body, out, ins, scratch=(), outs=None, flops=1 << 20, limit=40 << 20):
    return pl.pallas_call(
        body,
        out_shape=out,
        in_specs=ins,
        out_specs=outs if outs is not None else jax.tree.map(lambda _: VMEM, out),
        scratch_shapes=list(scratch),
        cost_estimate=pl.CostEstimate(flops=flops, bytes_accessed=1 << 20, transcendentals=0),
        compiler_params=pltpu.CompilerParams(vmem_limit_bytes=limit),
    )


def iota(shape, dim):
    return lax.broadcasted_iota(jnp.int32, shape, dim)


def to_lanes(col):
    n = col.shape[0]
    here = iota((n, LANES), 0) == iota((n, LANES), 1)
    return jnp.sum(jnp.where(here, jnp.broadcast_to(col, (n, LANES)), 0.0), axis=0, keepdims=True)


def to_rows(row, n):
    here = iota((n, LANES), 0) == iota((n, LANES), 1)
    return jnp.sum(jnp.where(here, jnp.broadcast_to(row, (n, LANES)), 0.0), axis=1, keepdims=True)


def norm_kernel(at, hid, gain, weights, *refs):
    more = refs[:-3]
    normed, sumsq, acc = refs[-3:]
    tok, feats = hid.shape
    line = at[0] // LANES
    nb = tok // LANES
    sumsq[...] = more[0][...] if more else jnp.zeros_like(sumsq)
    for b in range(nb):
        rows = pl.ds(b * LANES, LANES)
        folded = None
        for t in range(feats // LANES):
            lanes = pl.ds(t * LANES, LANES)
            raw = hid[rows, lanes].astype(F32)
            folded = raw * raw if folded is None else folded + raw * raw
            normed[rows, lanes] = (raw * gain[pl.ds(line + t, 1), :]).astype(BF16)
        sumsq[b : b + 1, :] += to_lanes(jnp.sum(folded, axis=1, keepdims=True))
    out = jnp.dot(normed[...], weights[...], preferred_element_type=F32)
    acc[...] = out + more[1][...] if more else out


def part_of(at, rows, blk):
    q = blk.shape[0]
    cols = pl.ds(pl.multiple_of(at * q, LANES), q)
    return jnp.dot(rows[:, cols], blk[...], preferred_element_type=F32)


def early_kernel(at, mine, other, a0, b0, out):
    out[...] = part_of(at[0], mine, a0) + part_of(at[0], other, b0)


def middle_kernel(at, mine, total, a1, a2, a3, out):
    acc = total[...]
    for k, blk in enumerate((a1, a2, a3)):
        acc = acc + part_of(at[k + 1], mine, blk)
    out[...] = acc


def late_kernel(at, other, total, b1, b2, b3, out_k, out_v):
    head = out_k.shape[1]
    acc = total[...]
    for k, blk in enumerate((b1, b2, b3)):
        acc = acc + part_of(at[k + 1], other, blk)
    out_k[...] = acc[:, :head].astype(BF16)
    out_v[...] = acc[:, head:].astype(BF16)


def inverse_rms(sqs, full_width):
    sumsq = sqs[0][...]
    for sq in sqs[1:]:
        sumsq = sumsq + sq[...]
    return lax.rsqrt(sumsq / full_width + 1e-05)


def score_kernel(full_width, scale_by, first, *refs):
    n_off = (len(refs) - 10) // 2
    acc, parts, sqs = refs[0], refs[1 : 1 + n_off], refs[1 + n_off : 2 + 2 * n_off]
    cos, sin, q, limit, expo, stats, keys, rows_of = refs[2 + 2 * n_off :]
    tok, head = keys.shape
    window = q.shape[0]
    for j in range(q.shape[1] // head):
        rows_of[j * window : (j + 1) * window, :] = q[:, j * head : (j + 1) * head]
    inv = inverse_rms(sqs, full_width)
    for b in range(tok // LANES):
        rows = pl.ds(b * LANES, LANES)
        k = acc[rows, :head]
        for p in parts:
            k = k + p[rows, :].astype(F32)
        k = k * to_rows(inv[b : b + 1, :], LANES)
        keys[rows, :] = (k * cos[rows, :] + pltpu.roll(k, head // 2, 1) * sin[rows, :]).astype(BF16)
    scores = lax.dot_general(
        keys[...], rows_of[...], (((1,), (1,)), ((), ())), preferred_element_type=F32
    ) * scale_by
    open_to = tok - window
    token = first[0] + open_to + iota((window, 1), 0)
    tail = jnp.where(token <= limit[...], scores[open_to:, :], MASKED)
    body = scores[:open_to, :]
    top = jnp.maximum(
        jnp.max(body, axis=0, keepdims=True), jnp.max(tail, axis=0, keepdims=True)
    )
    body, tail = jnp.exp(body - top), jnp.exp(tail - top)
    expo[:open_to, :] = body
    expo[open_to:, :] = tail
    own = jnp.sum(body, axis=0, keepdims=True) + jnp.sum(tail, axis=0, keepdims=True)
    for d in range(stats.shape[0]):
        stats[d, 0:1, :] = top
        stats[d, 1:2, :] = own


def value_kernel(full_width, *refs):
    n_off = (len(refs) - 3) // 2
    acc, parts, sqs, out = refs[0], refs[1 : 1 + n_off], refs[1 + n_off : 2 + 2 * n_off], refs[-1]
    head = acc.shape[1] // 2
    inv = inverse_rms(sqs, full_width)
    out[...] = jnp.zeros_like(out)
    for b in range(acc.shape[0] // LANES):
        rows = pl.ds(b * LANES, LANES)
        v = acc[rows, head:]
        for p in parts:
            v = v + p[rows, :].astype(F32)
        total = to_lanes(jnp.sum(jnp.abs(v), axis=1, keepdims=True))
        out[b : b + 1, :] = total * (1.0 / head) * inv[b : b + 1, :]


def widen(column, below, above, lane, halfspan):
    pooled = column
    for shift in range(1, REACH + 1):
        right = pltpu.roll(jnp.where(lane < shift, below, column), LANES - shift, 1)
        left = pltpu.roll(jnp.where(lane >= LANES - shift, above, column), shift, 1)
        pooled = jnp.where(
            shift <= halfspan, jnp.maximum(jnp.maximum(pooled, right), left), pooled
        )
    return pooled


def pool_kernel(window, sizes, got, mine, expo, vmag, win, spread):
    tok = expo.shape[0]
    nb = tok // LANES
    row_top = got[0, 0:1, :]
    for d in range(1, got.shape[0]):
        row_top = jnp.maximum(row_top, got[d, 0:1, :])
    row_total = jnp.zeros_like(row_top)
    for d in range(got.shape[0]):
        row_total = row_total + got[d, 1:2, :] * jnp.exp(got[d, 0:1, :] - row_top)
    weight = jnp.exp(mine[0, 0:1, :] - row_top) / row_total
    weight = jnp.where(win[...] >= window - sizes[0], weight, 0.0)
    height = vmag.shape[0]
    line = iota((height, LANES), 0)
    lane = iota((height, LANES), 1)
    column = jnp.zeros((height, LANES), F32)
    for b in range(nb):
        mass = jnp.sum(expo[b * LANES : (b + 1) * LANES, :] * weight, axis=1, keepdims=True)
        column = jnp.where(line == b, jnp.broadcast_to(to_lanes(mass), (height, LANES)), column)
    column = column * vmag[...]
    below, above = pltpu.roll(column, height - 1, 0), pltpu.roll(column, 1, 0)
    halfspan = lax.shift_right_arithmetic(sizes[1] - 1, 1)
    pooled = widen(column, below, above, lane, halfspan)
    place = line * LANES + lane
    inner = (place >= REACH) & (place < tok - REACH)
    sums = to_lanes(jnp.sum(jnp.where(inner, pooled, 0.0), axis=1, keepdims=True))
    flat = lane[0:1, :]
    last = pltpu.roll(column[nb - 1 : nb, :], 2 * EDGE, 1)
    said = jnp.where(flat < EDGE, column[0:1, :], jnp.where(flat < 2 * EDGE, last, pltpu.roll(sums, 2 * EDGE, 1)))
    spread[...] = jnp.broadcast_to(said, spread.shape)


def rank_kernel(nb, sizes, said, blocks, share):
    v = said[...]
    n = v.shape[0]
    line, lane = iota(v.shape, 0), iota(v.shape, 1)
    following = pltpu.roll(v, n - 1, 0)
    seam = jnp.where(lane < EDGE, pltpu.roll(v, LANES - EDGE, 1), pltpu.roll(following, EDGE, 1))
    seam = jnp.where(lane < 2 * EDGE, seam, 0.0)
    end = line == n - 1
    apart = LANES // 2
    halfspan = lax.shift_right_arithmetic(sizes[1] - 1, 1)
    both = jnp.where(end & (lane >= EDGE), 0.0, seam) + pltpu.roll(
        jnp.where(end & (lane < EDGE), 0.0, seam), apart, 1
    )
    pooled = both
    for shift in range(1, REACH + 1):
        near = jnp.maximum(pltpu.roll(both, shift, 1), pltpu.roll(both, LANES - shift, 1))
        pooled = jnp.where(shift <= halfspan, jnp.maximum(pooled, near), pooled)
    tail = (lane >= EDGE - REACH) & (lane < EDGE)
    lead = (lane >= apart + EDGE) & (lane < apart + EDGE + REACH)
    tail = jnp.sum(jnp.where(tail, pooled, 0.0), axis=1, keepdims=True)
    lead = jnp.sum(jnp.where(lead, pooled, 0.0), axis=1, keepdims=True)
    lead = pltpu.roll(jnp.broadcast_to(lead, v.shape), 1, 0)
    b = pltpu.roll(v, LANES - 2 * EDGE, 1)
    b = b + jnp.where(lane == 0, lead, 0.0) + jnp.where(lane == nb - 1, tail, 0.0)
    b = jnp.where(lane < nb, b, 0.0)
    own = jnp.sum(jnp.where(line == sizes[2], b, 0.0), axis=0, keepdims=True)
    blocks[...] = own[:, :nb]
    place = line * nb + lane
    rank = jnp.zeros(v.shape, jnp.int32)

    def turned(t, k):
        return jnp.where(lane >= k, pltpu.roll(t, k, 1), pltpu.roll(t, LANES + k - nb, 1)) if k else t

    for k in range(nb):
        bk, pk = turned(b, k), turned(place, k)
        for m in range(n):
            bm, pm = (pltpu.roll(bk, m, 0), pltpu.roll(pk, m, 0)) if m else (bk, pk)
            rank = rank + jnp.where((bm > b) | ((bm == b) & (pm < place)), 1, 0)

    def add(t):
        return jnp.sum(jnp.sum(t, axis=1, keepdims=True), axis=0, keepdims=True)

    kept = jnp.where((lane < nb) & (rank < sizes[0]), b, 0.0)
    share[...] = add(kept) / add(b)


def local(
    hidden, gain, key_matrix, value_matrix, queries, window_len, kernel_width, kept_block_count
):
    tok, feats = hidden.shape
    full_width = gain.shape[0]
    head = key_matrix.shape[1]
    n_seq, n_head = lax.axis_size("seq"), lax.axis_size("head")
    n_x = n_head // CORES
    s, h = lax.axis_index("seq"), lax.axis_index("head")
    x, c = h // CORES, h % CORES
    i = s % GROUP
    q = feats // GROUP
    total_tokens = tok * n_seq
    offsets = range(1, n_x)

    def shift_x(offset):
        return [
            (a * CORES + b, (a + offset) % n_x * CORES + b) for a in range(n_x) for b in range(CORES)
        ]

    def flip(bit):
        return [(j, j ^ bit) for j in range(n_seq)]

    def rows_at(start, count):
        return jnp.concatenate(
            [lax.dynamic_slice_in_dim(m, start, count) for m in (key_matrix, value_matrix)], axis=1
        )

    def cross(o, block):
        chip = (x - o) % n_x
        return [
            lax.ppermute(
                rows_at((chip * CORES + (c ^ part)) * feats + block * q, q), "head", shift_x(-o)
            )
            for part in range(CORES)
        ]

    firsts = [cross(o, i) for o in offsets]
    seconds = [cross(o, 3 - i) for o in offsets]
    swapped = lax.ppermute(hidden, "head", [(j, j ^ 1) for j in range(n_head)])
    blocks = [
        [
            [firsts[o - 1][part]]
            + [lax.ppermute(firsts[o - 1][part], "seq", flip(bit)) for bit in (1, 2)]
            + [seconds[o - 1][part]]
            for part in range(CORES)
        ]
        for o in offsets
    ]

    lines = -(-(tok // LANES) // 8) * 8
    gain_lines = gain.reshape(full_width // LANES, LANES)

    def norm(start, rows, more):
        weights = rows_at(start, feats)
        return call(
            norm_kernel,
            [sds((tok, feats), BF16), sds((lines, LANES), F32), sds((tok, 2 * head), F32)],
            [SMEM] + [VMEM] * (3 + len(more)),
            flops=1 << 30,
        )(start.reshape(1), rows, gain_lines, weights, *more)

    mine, sumsq, acc = norm(h * feats, hidden, ())
    other, sumsq, acc = norm((h ^ 1) * feats, swapped, (sumsq, acc))
    sqs = [sumsq] + [lax.ppermute(sumsq, "head", shift_x(o)) for o in offsets]

    parts_k, parts_v = [], []
    slabs = jnp.stack([i ^ k for k in range(GROUP)])
    wide, thin = sds((tok, 2 * head), F32), sds((tok, head), BF16)
    for o in offsets:
        half_0, half_1 = blocks[o - 1]
        part = call(early_kernel, wide, [SMEM] + [VMEM] * 4, flops=1 << 29)(
            slabs, mine, other, half_0[0], half_1[0]
        )
        part = call(middle_kernel, wide, [SMEM] + [VMEM] * 5, flops=1 << 29)(
            slabs, mine, part, *half_0[1:]
        )
        part_k, part_v = call(
            late_kernel, [thin, thin], [SMEM] + [VMEM] * 5, flops=1 << 29
        )(slabs, other, part, *half_1[1:])
        parts_k.append(lax.ppermute(part_k, "head", shift_x(o)))
        parts_v.append(lax.ppermute(part_v, "head", shift_x(o)))

    half = head // 2
    freq = 500000.0 ** (-(jnp.arange(half).astype(F32) * 2.0) / head)
    token = s * tok + jnp.arange(tok)
    angle = token.astype(F32)[:, None] * freq[None, :]
    cos, sin = jnp.cos(angle), jnp.sin(angle)
    cos = jnp.concatenate([cos, cos], axis=1)
    sin = jnp.concatenate([-sin, sin], axis=1)

    window = queries.shape[0]
    group_heads = queries.shape[1] // head
    rows = window * group_heads
    row_window = (jnp.arange(rows) % window).astype(jnp.int32)[None, :]
    limit = total_tokens - window + row_window
    expo, stats = call(
        functools.partial(score_kernel, full_width, head ** (-0.5)),
        [sds((tok, rows), F32), sds((n_seq, 2, rows), F32)],
        [SMEM] + [VMEM] * (6 + 2 * len(offsets)),
        scratch=[pltpu.VMEM((tok, head), BF16), pltpu.VMEM((rows, head), BF16)],
        flops=1 << 28,
    )((s * tok).reshape(1), acc, *parts_k, *sqs, cos, sin, queries, limit)
    got = lax.all_to_all(stats, "seq", 0, 0, tiled=True)
    nb = tok // BLK
    vmag = call(
        functools.partial(value_kernel, full_width),
        sds((lines, LANES), F32),
        [VMEM] * (2 + 2 * len(offsets)),
        flops=1 << 28,
    )(acc, *parts_v, *sqs)
    spread = call(
        functools.partial(pool_kernel, window),
        sds((n_seq, LANES), F32),
        [SMEM] + [VMEM] * 5,
        flops=1 << 26,
    )(jnp.concatenate([window_len, kernel_width]), got, stats, expo, vmag, row_window)
    said = lax.all_to_all(spread, "seq", 0, 0, tiled=True)
    local_blocks, fraction = call(
        functools.partial(rank_kernel, nb),
        [sds((1, nb), F32), sds((1, 1), F32)],
        [SMEM, VMEM],
        flops=1 << 20,
    )(jnp.concatenate([kept_block_count, kernel_width, s.reshape(1)]), said)
    return (local_blocks, fraction.reshape(1))


def solution(mesh):
    return jax.shard_map(
        local,
        mesh=mesh,
        in_specs=(
            P("seq", "head"),
            P(),
            P(None, "head"),
            P(None, "head"),
            P(None, "head"),
            P("head"),
            P("head"),
            P("head"),
        ),
        out_specs=(P("head", "seq"), P("head")),
        check_vma=False,
    )
```

```python
import functools

import jax
import jax.numpy as jnp
from jax import lax
from jax.experimental import pallas as pl
from jax.experimental.pallas import tpu as pltpu
from jax.sharding import PartitionSpec as P

BLK = 128
LANES = 128
KERNEL_LIMIT = 15
REACH = (KERNEL_LIMIT - 1) // 2
EDGE = 16
CORES = 2
GROUP = 4
MASKED = -1e30

VMEM = pl.BlockSpec(memory_space=pltpu.VMEM)
SMEM = pl.BlockSpec(memory_space=pltpu.SMEM)
F32, BF16 = jnp.float32, jnp.bfloat16


def sds(shape, dtype):
    return jax.ShapeDtypeStruct(shape, dtype)


def call(body, out, ins, scratch=(), outs=None, flops=1 << 20, limit=40 << 20):
    return pl.pallas_call(
        body,
        out_shape=out,
        in_specs=ins,
        out_specs=outs if outs is not None else jax.tree.map(lambda _: VMEM, out),
        scratch_shapes=list(scratch),
        cost_estimate=pl.CostEstimate(flops=flops, bytes_accessed=1 << 20, transcendentals=0),
        compiler_params=pltpu.CompilerParams(vmem_limit_bytes=limit),
    )


def iota(shape, dim):
    return lax.broadcasted_iota(jnp.int32, shape, dim)


def to_lanes(col):
    n = col.shape[0]
    here = iota((n, LANES), 0) == iota((n, LANES), 1)
    return jnp.sum(jnp.where(here, jnp.broadcast_to(col, (n, LANES)), 0.0), axis=0, keepdims=True)


def to_rows(row, n):
    here = iota((n, LANES), 0) == iota((n, LANES), 1)
    return jnp.sum(jnp.where(here, jnp.broadcast_to(row, (n, LANES)), 0.0), axis=1, keepdims=True)


def norm_kernel(at, hid, gain, weights, *refs):
    more = refs[:-3]
    normed, sumsq, acc = refs[-3:]
    tok, feats = hid.shape
    line = at[0] // LANES
    nb = tok // LANES
    sumsq[...] = more[0][...] if more else jnp.zeros_like(sumsq)
    for b in range(nb):
        rows = pl.ds(b * LANES, LANES)
        folded = None
        for t in range(feats // LANES):
            lanes = pl.ds(t * LANES, LANES)
            raw = hid[rows, lanes].astype(F32)
            folded = raw * raw if folded is None else folded + raw * raw
            normed[rows, lanes] = (raw * gain[pl.ds(line + t, 1), :]).astype(BF16)
        sumsq[b : b + 1, :] += to_lanes(jnp.sum(folded, axis=1, keepdims=True))
    out = jnp.dot(normed[...], weights[...], preferred_element_type=F32)
    acc[...] = out + more[1][...] if more else out


def part_of(at, rows, blk):
    q = blk.shape[0]
    cols = pl.ds(pl.multiple_of(at * q, LANES), q)
    return jnp.dot(rows[:, cols], blk[...], preferred_element_type=F32)


def early_kernel(at, mine, other, a0, b0, out):
    out[...] = part_of(at[0], mine, a0) + part_of(at[0], other, b0)


def middle_kernel(at, mine, total, a1, a2, a3, out):
    acc = total[...]
    for k, blk in enumerate((a1, a2, a3)):
        acc = acc + part_of(at[k + 1], mine, blk)
    out[...] = acc


def late_kernel(at, other, total, b1, b2, b3, out_k, out_v):
    head = out_k.shape[1]
    acc = total[...]
    for k, blk in enumerate((b1, b2, b3)):
        acc = acc + part_of(at[k + 1], other, blk)
    out_k[...] = acc[:, :head].astype(BF16)
    out_v[...] = acc[:, head:].astype(BF16)


def inverse_rms(sqs, full_width):
    sumsq = sqs[0][...]
    for sq in sqs[1:]:
        sumsq = sumsq + sq[...]
    return lax.rsqrt(sumsq / full_width + 1e-05)


def score_kernel(full_width, scale_by, first, *refs):
    n_off = (len(refs) - 10) // 2
    acc, parts, sqs = refs[0], refs[1 : 1 + n_off], refs[1 + n_off : 2 + 2 * n_off]
    cos, sin, q, limit, expo, stats, keys, rows_of = refs[2 + 2 * n_off :]
    tok, head = keys.shape
    window = q.shape[0]
    for j in range(q.shape[1] // head):
        rows_of[j * window : (j + 1) * window, :] = q[:, j * head : (j + 1) * head]
    inv = inverse_rms(sqs, full_width)
    for b in range(tok // LANES):
        rows = pl.ds(b * LANES, LANES)
        k = acc[rows, :head]
        for p in parts:
            k = k + p[rows, :].astype(F32)
        k = k * to_rows(inv[b : b + 1, :], LANES)
        keys[rows, :] = (k * cos[rows, :] + pltpu.roll(k, head // 2, 1) * sin[rows, :]).astype(BF16)
    scores = lax.dot_general(
        keys[...], rows_of[...], (((1,), (1,)), ((), ())), preferred_element_type=F32
    ) * scale_by
    open_to = tok - window
    token = first[0] + open_to + iota((window, 1), 0)
    tail = jnp.where(token <= limit[...], scores[open_to:, :], MASKED)
    body = scores[:open_to, :]
    top = jnp.maximum(
        jnp.max(body, axis=0, keepdims=True), jnp.max(tail, axis=0, keepdims=True)
    )
    body, tail = jnp.exp(body - top), jnp.exp(tail - top)
    expo[:open_to, :] = body
    expo[open_to:, :] = tail
    own = jnp.sum(body, axis=0, keepdims=True) + jnp.sum(tail, axis=0, keepdims=True)
    for d in range(stats.shape[0]):
        stats[d, 0:1, :] = top
        stats[d, 1:2, :] = own


def value_kernel(full_width, *refs):
    n_off = (len(refs) - 3) // 2
    acc, parts, sqs, out = refs[0], refs[1 : 1 + n_off], refs[1 + n_off : 2 + 2 * n_off], refs[-1]
    head = acc.shape[1] // 2
    inv = inverse_rms(sqs, full_width)
    out[...] = jnp.zeros_like(out)
    for b in range(acc.shape[0] // LANES):
        rows = pl.ds(b * LANES, LANES)
        v = acc[rows, head:]
        for p in parts:
            v = v + p[rows, :].astype(F32)
        total = to_lanes(jnp.sum(jnp.abs(v), axis=1, keepdims=True))
        out[b : b + 1, :] = total * (1.0 / head) * inv[b : b + 1, :]


def widen(column, below, above, lane, halfspan):
    pooled = column
    for shift in range(1, REACH + 1):
        right = pltpu.roll(jnp.where(lane < shift, below, column), LANES - shift, 1)
        left = pltpu.roll(jnp.where(lane >= LANES - shift, above, column), shift, 1)
        pooled = jnp.where(
            shift <= halfspan, jnp.maximum(jnp.maximum(pooled, right), left), pooled
        )
    return pooled


def pool_kernel(window, sizes, got, mine, expo, vmag, win, spread):
    tok = expo.shape[0]
    nb = tok // LANES
    row_top = got[0, 0:1, :]
    for d in range(1, got.shape[0]):
        row_top = jnp.maximum(row_top, got[d, 0:1, :])
    row_total = jnp.zeros_like(row_top)
    for d in range(got.shape[0]):
        row_total = row_total + got[d, 1:2, :] * jnp.exp(got[d, 0:1, :] - row_top)
    weight = jnp.exp(mine[0, 0:1, :] - row_top) / row_total
    weight = jnp.where(win[...] >= window - sizes[0], weight, 0.0)
    height = vmag.shape[0]
    line = iota((height, LANES), 0)
    lane = iota((height, LANES), 1)
    column = jnp.zeros((height, LANES), F32)
    for b in range(nb):
        mass = jnp.sum(expo[b * LANES : (b + 1) * LANES, :] * weight, axis=1, keepdims=True)
        column = jnp.where(line == b, jnp.broadcast_to(to_lanes(mass), (height, LANES)), column)
    column = column * vmag[...]
    below, above = pltpu.roll(column, height - 1, 0), pltpu.roll(column, 1, 0)
    halfspan = lax.shift_right_arithmetic(sizes[1] - 1, 1)
    pooled = widen(column, below, above, lane, halfspan)
    place = line * LANES + lane
    inner = (place >= REACH) & (place < tok - REACH)
    sums = to_lanes(jnp.sum(jnp.where(inner, pooled, 0.0), axis=1, keepdims=True))
    flat = lane[0:1, :]
    last = pltpu.roll(column[nb - 1 : nb, :], 2 * EDGE, 1)
    said = jnp.where(flat < EDGE, column[0:1, :], jnp.where(flat < 2 * EDGE, last, pltpu.roll(sums, 2 * EDGE, 1)))
    spread[...] = jnp.broadcast_to(said, spread.shape)


def rank_kernel(nb, sizes, said, blocks, share):
    v = said[...]
    n = v.shape[0]
    line, lane = iota(v.shape, 0), iota(v.shape, 1)
    following = pltpu.roll(v, n - 1, 0)
    seam = jnp.where(lane < EDGE, pltpu.roll(v, LANES - EDGE, 1), pltpu.roll(following, EDGE, 1))
    seam = jnp.where(lane < 2 * EDGE, seam, 0.0)
    end = line == n - 1
    apart = LANES // 2
    halfspan = lax.shift_right_arithmetic(sizes[1] - 1, 1)
    both = jnp.where(end & (lane >= EDGE), 0.0, seam) + pltpu.roll(
        jnp.where(end & (lane < EDGE), 0.0, seam), apart, 1
    )
    pooled = both
    for shift in range(1, REACH + 1):
        near = jnp.maximum(pltpu.roll(both, shift, 1), pltpu.roll(both, LANES - shift, 1))
        pooled = jnp.where(shift <= halfspan, jnp.maximum(pooled, near), pooled)
    tail = (lane >= EDGE - REACH) & (lane < EDGE)
    lead = (lane >= apart + EDGE) & (lane < apart + EDGE + REACH)
    tail = jnp.sum(jnp.where(tail, pooled, 0.0), axis=1, keepdims=True)
    lead = jnp.sum(jnp.where(lead, pooled, 0.0), axis=1, keepdims=True)
    lead = pltpu.roll(jnp.broadcast_to(lead, v.shape), 1, 0)
    b = pltpu.roll(v, LANES - 2 * EDGE, 1)
    b = b + jnp.where(lane == 0, lead, 0.0) + jnp.where(lane == nb - 1, tail, 0.0)
    b = jnp.where(lane < nb, b, 0.0)
    own = jnp.sum(jnp.where(line == sizes[2], b, 0.0), axis=0, keepdims=True)
    blocks[...] = own[:, :nb]
    place = line * nb + lane
    rank = jnp.zeros(v.shape, jnp.int32)

    def turned(t, k):
        return jnp.where(lane >= k, pltpu.roll(t, k, 1), pltpu.roll(t, LANES + k - nb, 1)) if k else t

    for k in range(nb):
        bk, pk = turned(b, k), turned(place, k)
        for m in range(n):
            bm, pm = (pltpu.roll(bk, m, 0), pltpu.roll(pk, m, 0)) if m else (bk, pk)
            rank = rank + jnp.where((bm > b) | ((bm == b) & (pm < place)), 1, 0)

    def add(t):
        return jnp.sum(jnp.sum(t, axis=1, keepdims=True), axis=0, keepdims=True)

    kept = jnp.where((lane < nb) & (rank < sizes[0]), b, 0.0)
    share[...] = add(kept) / add(b)


def local(
    hidden, gain, key_matrix, value_matrix, queries, window_len, kernel_width, kept_block_count
):
    tok, feats = hidden.shape
    full_width = gain.shape[0]
    head = key_matrix.shape[1]
    n_seq, n_head = lax.axis_size("seq"), lax.axis_size("head")
    n_x = n_head // CORES
    s, h = lax.axis_index("seq"), lax.axis_index("head")
    x, c = h // CORES, h % CORES
    i = s % GROUP
    q = feats // GROUP
    total_tokens = tok * n_seq
    offsets = range(1, n_x)

    def shift_x(offset):
        return [
            (a * CORES + b, (a + offset) % n_x * CORES + b) for a in range(n_x) for b in range(CORES)
        ]

    def flip(bit):
        return [(j, j ^ bit) for j in range(n_seq)]

    weights = [key_matrix, value_matrix]

    def rows_at(start, count):
        rows = jnp.concatenate(
            [lax.dynamic_slice_in_dim(m, start, count) for m in weights], axis=1
        )
        weights[0], weights[1], rows = lax.optimization_barrier((*weights, rows))
        return rows

    def cross(o, block):
        chip = (x - o) % n_x
        return [
            lax.ppermute(
                rows_at((chip * CORES + (c ^ part)) * feats + block * q, q), "head", shift_x(-o)
            )
            for part in range(CORES)
        ]

    firsts = [cross(o, i) for o in offsets]
    seconds = [cross(o, 3 - i) for o in offsets]
    swapped = lax.ppermute(hidden, "head", [(j, j ^ 1) for j in range(n_head)])
    blocks = [
        [
            [firsts[o - 1][part]]
            + [lax.ppermute(firsts[o - 1][part], "seq", flip(bit)) for bit in (1, 2)]
            + [seconds[o - 1][part]]
            for part in range(CORES)
        ]
        for o in offsets
    ]

    lines = -(-(tok // LANES) // 8) * 8
    gain_lines = gain.reshape(full_width // LANES, LANES)

    def norm(start, rows, more):
        own = rows_at(start, feats)
        return call(
            norm_kernel,
            [sds((tok, feats), BF16), sds((lines, LANES), F32), sds((tok, 2 * head), F32)],
            [SMEM] + [VMEM] * (3 + len(more)),
            flops=1 << 30,
        )(start.reshape(1), rows, gain_lines, own, *more)

    mine, sumsq, acc = norm(h * feats, hidden, ())
    other, sumsq, acc = norm((h ^ 1) * feats, swapped, (sumsq, acc))
    sqs = [sumsq] + [lax.ppermute(sumsq, "head", shift_x(o)) for o in offsets]

    parts_k, parts_v = [], []
    slabs = jnp.stack([i ^ k for k in range(GROUP)])
    wide, thin = sds((tok, 2 * head), F32), sds((tok, head), BF16)
    for o in offsets:
        half_0, half_1 = blocks[o - 1]
        part = call(early_kernel, wide, [SMEM] + [VMEM] * 4, flops=1 << 29)(
            slabs, mine, other, half_0[0], half_1[0]
        )
        part = call(middle_kernel, wide, [SMEM] + [VMEM] * 5, flops=1 << 29)(
            slabs, mine, part, *half_0[1:]
        )
        part_k, part_v = call(
            late_kernel, [thin, thin], [SMEM] + [VMEM] * 5, flops=1 << 29
        )(slabs, other, part, *half_1[1:])
        parts_k.append(lax.ppermute(part_k, "head", shift_x(o)))
        parts_v.append(lax.ppermute(part_v, "head", shift_x(o)))

    half = head // 2
    freq = 500000.0 ** (-(jnp.arange(half).astype(F32) * 2.0) / head)
    token = s * tok + jnp.arange(tok)
    angle = token.astype(F32)[:, None] * freq[None, :]
    cos, sin = jnp.cos(angle), jnp.sin(angle)
    cos = jnp.concatenate([cos, cos], axis=1)
    sin = jnp.concatenate([-sin, sin], axis=1)

    window = queries.shape[0]
    group_heads = queries.shape[1] // head
    rows = window * group_heads
    row_window = (jnp.arange(rows) % window).astype(jnp.int32)[None, :]
    limit = total_tokens - window + row_window
    expo, stats = call(
        functools.partial(score_kernel, full_width, head ** (-0.5)),
        [sds((tok, rows), F32), sds((n_seq, 2, rows), F32)],
        [SMEM] + [VMEM] * (6 + 2 * len(offsets)),
        scratch=[pltpu.VMEM((tok, head), BF16), pltpu.VMEM((rows, head), BF16)],
        flops=1 << 28,
    )((s * tok).reshape(1), acc, *parts_k, *sqs, cos, sin, queries, limit)
    got = lax.all_to_all(stats, "seq", 0, 0, tiled=True)
    nb = tok // BLK
    vmag = call(
        functools.partial(value_kernel, full_width),
        sds((lines, LANES), F32),
        [VMEM] * (2 + 2 * len(offsets)),
        flops=1 << 28,
    )(acc, *parts_v, *sqs)
    spread = call(
        functools.partial(pool_kernel, window),
        sds((n_seq, LANES), F32),
        [SMEM] + [VMEM] * 5,
        flops=1 << 26,
    )(jnp.concatenate([window_len, kernel_width]), got, stats, expo, vmag, row_window)
    said = lax.all_to_all(spread, "seq", 0, 0, tiled=True)
    local_blocks, fraction = call(
        functools.partial(rank_kernel, nb),
        [sds((1, nb), F32), sds((1, 1), F32)],
        [SMEM, VMEM],
        flops=1 << 20,
    )(jnp.concatenate([kept_block_count, kernel_width, s.reshape(1)]), said)
    return (local_blocks, fraction.reshape(1))


def solution(mesh):
    return jax.shard_map(
        local,
        mesh=mesh,
        in_specs=(
            P("seq", "head"),
            P(),
            P(None, "head"),
            P(None, "head"),
            P(None, "head"),
            P("head"),
            P("head"),
            P("head"),
        ),
        out_specs=(P("head", "seq"), P("head")),
        check_vma=False,
    )
```

```python
import functools

import jax
import jax.numpy as jnp
from jax import lax
from jax.experimental import pallas as pl
from jax.experimental.pallas import tpu as pltpu
from jax.sharding import PartitionSpec as P

BLK = 128
LANES = 128
KERNEL_LIMIT = 15
REACH = (KERNEL_LIMIT - 1) // 2
EDGE = 16
CORES = 2
GROUP = 4
MASKED = -1e30

VMEM = pl.BlockSpec(memory_space=pltpu.VMEM)
SMEM = pl.BlockSpec(memory_space=pltpu.SMEM)
F32, BF16 = jnp.float32, jnp.bfloat16


def sds(shape, dtype):
    return jax.ShapeDtypeStruct(shape, dtype)


def call(body, out, ins, scratch=(), outs=None, flops=1 << 20, limit=40 << 20):
    return pl.pallas_call(
        body,
        out_shape=out,
        in_specs=ins,
        out_specs=outs if outs is not None else jax.tree.map(lambda _: VMEM, out),
        scratch_shapes=list(scratch),
        cost_estimate=pl.CostEstimate(flops=flops, bytes_accessed=1 << 20, transcendentals=0),
        compiler_params=pltpu.CompilerParams(vmem_limit_bytes=limit),
    )


def iota(shape, dim):
    return lax.broadcasted_iota(jnp.int32, shape, dim)


def to_lanes(col):
    n = col.shape[0]
    here = iota((n, LANES), 0) == iota((n, LANES), 1)
    return jnp.sum(jnp.where(here, jnp.broadcast_to(col, (n, LANES)), 0.0), axis=0, keepdims=True)


def to_rows(row, n):
    here = iota((n, LANES), 0) == iota((n, LANES), 1)
    return jnp.sum(jnp.where(here, jnp.broadcast_to(row, (n, LANES)), 0.0), axis=1, keepdims=True)


def norm_kernel(at, hid, gain, weights, *refs):
    more = refs[:-3]
    normed, sumsq, acc = refs[-3:]
    b = pl.program_id(0)
    line = at[0]

    @pl.when(b == 0)
    def _():
        sumsq[...] = more[0][...] if more else jnp.zeros_like(sumsq)

    folded = None
    for t in range(hid.shape[1] // LANES):
        lanes = pl.ds(t * LANES, LANES)
        raw = hid[:, lanes].astype(F32)
        folded = raw * raw if folded is None else folded + raw * raw
        normed[:, lanes] = (raw * gain[pl.ds(line + t, 1), :]).astype(BF16)
    sumsq[pl.ds(b, 1), :] += to_lanes(jnp.sum(folded, axis=1, keepdims=True))
    out = jnp.dot(normed[...], weights[...], preferred_element_type=F32)
    acc[...] = out + more[1][...] if more else out


def part_of(at, rows, blk):
    q = blk.shape[0]
    cols = pl.ds(pl.multiple_of(at * q, LANES), q)
    return jnp.dot(rows[:, cols], blk[...], preferred_element_type=F32)


def early_kernel(at, mine, other, a0, b0, out):
    out[...] = part_of(at[0], mine, a0) + part_of(at[0], other, b0)


def middle_kernel(at, mine, total, a1, a2, a3, out):
    acc = total[...]
    for k, blk in enumerate((a1, a2, a3)):
        acc = acc + part_of(at[k + 1], mine, blk)
    out[...] = acc


def late_kernel(at, other, total, b1, b2, b3, out_k, out_v):
    head = out_k.shape[1]
    acc = total[...]
    for k, blk in enumerate((b1, b2, b3)):
        acc = acc + part_of(at[k + 1], other, blk)
    out_k[...] = acc[:, :head].astype(BF16)
    out_v[...] = acc[:, head:].astype(BF16)


def inverse_rms(sqs, full_width):
    sumsq = sqs[0][...]
    for sq in sqs[1:]:
        sumsq = sumsq + sq[...]
    return lax.rsqrt(sumsq / full_width + 1e-05)


def score_kernel(full_width, scale_by, first, *refs):
    n_off = (len(refs) - 10) // 2
    acc, parts, sqs = refs[0], refs[1 : 1 + n_off], refs[1 + n_off : 2 + 2 * n_off]
    cos, sin, q, limit, expo, stats, keys, rows_of = refs[2 + 2 * n_off :]
    tok, head = keys.shape
    window = q.shape[0]
    for j in range(q.shape[1] // head):
        rows_of[j * window : (j + 1) * window, :] = q[:, j * head : (j + 1) * head]
    inv = inverse_rms(sqs, full_width)
    for b in range(tok // LANES):
        rows = pl.ds(b * LANES, LANES)
        k = acc[rows, :head]
        for p in parts:
            k = k + p[rows, :].astype(F32)
        k = k * to_rows(inv[b : b + 1, :], LANES)
        keys[rows, :] = (k * cos[rows, :] + pltpu.roll(k, head // 2, 1) * sin[rows, :]).astype(BF16)
    scores = lax.dot_general(
        keys[...], rows_of[...], (((1,), (1,)), ((), ())), preferred_element_type=F32
    ) * scale_by
    open_to = tok - window
    token = first[0] + open_to + iota((window, 1), 0)
    tail = jnp.where(token <= limit[...], scores[open_to:, :], MASKED)
    body = scores[:open_to, :]
    top = jnp.maximum(
        jnp.max(body, axis=0, keepdims=True), jnp.max(tail, axis=0, keepdims=True)
    )
    body, tail = jnp.exp(body - top), jnp.exp(tail - top)
    expo[:open_to, :] = body
    expo[open_to:, :] = tail
    own = jnp.sum(body, axis=0, keepdims=True) + jnp.sum(tail, axis=0, keepdims=True)
    for d in range(stats.shape[0]):
        stats[d, 0:1, :] = top
        stats[d, 1:2, :] = own


def value_kernel(full_width, *refs):
    n_off = (len(refs) - 3) // 2
    acc, parts, sqs, out = refs[0], refs[1 : 1 + n_off], refs[1 + n_off : 2 + 2 * n_off], refs[-1]
    head = acc.shape[1] // 2
    inv = inverse_rms(sqs, full_width)
    out[...] = jnp.zeros_like(out)
    for b in range(acc.shape[0] // LANES):
        rows = pl.ds(b * LANES, LANES)
        v = acc[rows, head:]
        for p in parts:
            v = v + p[rows, :].astype(F32)
        total = to_lanes(jnp.sum(jnp.abs(v), axis=1, keepdims=True))
        out[b : b + 1, :] = total * (1.0 / head) * inv[b : b + 1, :]


def widen(column, below, above, lane, halfspan):
    pooled = column
    for shift in range(1, REACH + 1):
        right = pltpu.roll(jnp.where(lane < shift, below, column), LANES - shift, 1)
        left = pltpu.roll(jnp.where(lane >= LANES - shift, above, column), shift, 1)
        pooled = jnp.where(
            shift <= halfspan, jnp.maximum(jnp.maximum(pooled, right), left), pooled
        )
    return pooled


def pool_kernel(window, sizes, got, mine, expo, vmag, win, spread):
    tok = expo.shape[0]
    nb = tok // LANES
    row_top = got[0, 0:1, :]
    for d in range(1, got.shape[0]):
        row_top = jnp.maximum(row_top, got[d, 0:1, :])
    row_total = jnp.zeros_like(row_top)
    for d in range(got.shape[0]):
        row_total = row_total + got[d, 1:2, :] * jnp.exp(got[d, 0:1, :] - row_top)
    weight = jnp.exp(mine[0, 0:1, :] - row_top) / row_total
    weight = jnp.where(win[...] >= window - sizes[0], weight, 0.0)
    height = vmag.shape[0]
    line = iota((height, LANES), 0)
    lane = iota((height, LANES), 1)
    column = jnp.zeros((height, LANES), F32)
    for b in range(nb):
        mass = jnp.sum(expo[b * LANES : (b + 1) * LANES, :] * weight, axis=1, keepdims=True)
        column = jnp.where(line == b, jnp.broadcast_to(to_lanes(mass), (height, LANES)), column)
    column = column * vmag[...]
    below, above = pltpu.roll(column, height - 1, 0), pltpu.roll(column, 1, 0)
    halfspan = lax.shift_right_arithmetic(sizes[1] - 1, 1)
    pooled = widen(column, below, above, lane, halfspan)
    place = line * LANES + lane
    inner = (place >= REACH) & (place < tok - REACH)
    sums = to_lanes(jnp.sum(jnp.where(inner, pooled, 0.0), axis=1, keepdims=True))
    flat = lane[0:1, :]
    last = pltpu.roll(column[nb - 1 : nb, :], 2 * EDGE, 1)
    said = jnp.where(flat < EDGE, column[0:1, :], jnp.where(flat < 2 * EDGE, last, pltpu.roll(sums, 2 * EDGE, 1)))
    spread[...] = jnp.broadcast_to(said, spread.shape)


def rank_kernel(nb, sizes, said, blocks, share):
    v = said[...]
    n = v.shape[0]
    line, lane = iota(v.shape, 0), iota(v.shape, 1)
    following = pltpu.roll(v, n - 1, 0)
    seam = jnp.where(lane < EDGE, pltpu.roll(v, LANES - EDGE, 1), pltpu.roll(following, EDGE, 1))
    seam = jnp.where(lane < 2 * EDGE, seam, 0.0)
    end = line == n - 1
    apart = LANES // 2
    halfspan = lax.shift_right_arithmetic(sizes[1] - 1, 1)
    both = jnp.where(end & (lane >= EDGE), 0.0, seam) + pltpu.roll(
        jnp.where(end & (lane < EDGE), 0.0, seam), apart, 1
    )
    pooled = both
    for shift in range(1, REACH + 1):
        near = jnp.maximum(pltpu.roll(both, shift, 1), pltpu.roll(both, LANES - shift, 1))
        pooled = jnp.where(shift <= halfspan, jnp.maximum(pooled, near), pooled)
    tail = (lane >= EDGE - REACH) & (lane < EDGE)
    lead = (lane >= apart + EDGE) & (lane < apart + EDGE + REACH)
    tail = jnp.sum(jnp.where(tail, pooled, 0.0), axis=1, keepdims=True)
    lead = jnp.sum(jnp.where(lead, pooled, 0.0), axis=1, keepdims=True)
    lead = pltpu.roll(jnp.broadcast_to(lead, v.shape), 1, 0)
    b = pltpu.roll(v, LANES - 2 * EDGE, 1)
    b = b + jnp.where(lane == 0, lead, 0.0) + jnp.where(lane == nb - 1, tail, 0.0)
    b = jnp.where(lane < nb, b, 0.0)
    own = jnp.sum(jnp.where(line == sizes[2], b, 0.0), axis=0, keepdims=True)
    blocks[...] = own[:, :nb]
    place = line * nb + lane
    rank = jnp.zeros(v.shape, jnp.int32)

    def turned(t, k):
        return jnp.where(lane >= k, pltpu.roll(t, k, 1), pltpu.roll(t, LANES + k - nb, 1)) if k else t

    for k in range(nb):
        bk, pk = turned(b, k), turned(place, k)
        for m in range(n):
            bm, pm = (pltpu.roll(bk, m, 0), pltpu.roll(pk, m, 0)) if m else (bk, pk)
            rank = rank + jnp.where((bm > b) | ((bm == b) & (pm < place)), 1, 0)

    def add(t):
        return jnp.sum(jnp.sum(t, axis=1, keepdims=True), axis=0, keepdims=True)

    kept = jnp.where((lane < nb) & (rank < sizes[0]), b, 0.0)
    share[...] = add(kept) / add(b)


def local(
    hidden, gain, key_matrix, value_matrix, queries, window_len, kernel_width, kept_block_count
):
    tok, feats = hidden.shape
    full_width = gain.shape[0]
    head = key_matrix.shape[1]
    n_seq, n_head = lax.axis_size("seq"), lax.axis_size("head")
    n_x = n_head // CORES
    s, h = lax.axis_index("seq"), lax.axis_index("head")
    x, c = h // CORES, h % CORES
    i = s % GROUP
    q = feats // GROUP
    total_tokens = tok * n_seq
    offsets = range(1, n_x)

    def shift_x(offset):
        return [
            (a * CORES + b, (a + offset) % n_x * CORES + b) for a in range(n_x) for b in range(CORES)
        ]

    def flip(bit):
        return [(j, j ^ bit) for j in range(n_seq)]

    def rows_at(start, count):
        return jnp.concatenate(
            [lax.dynamic_slice_in_dim(m, start, count) for m in (key_matrix, value_matrix)], axis=1
        )

    def crossing(block):
        return [
            [
                rows_at(((x - o) % n_x * CORES + (c ^ part)) * feats + block * q, q)
                for part in range(CORES)
            ]
            for o in offsets
        ]

    def cross(rows):
        return [
            [lax.ppermute(rows[o - 1][part], "head", shift_x(-o)) for part in range(CORES)]
            for o in offsets
        ]

    firsts = cross(crossing(i))
    seconds = cross(crossing(3 - i))
    own = [rows_at(start * feats, feats) for start in (h, h ^ 1)]
    swapped = lax.ppermute(hidden, "head", [(j, j ^ 1) for j in range(n_head)])
    blocks = [
        [
            [firsts[o - 1][part]]
            + [lax.ppermute(firsts[o - 1][part], "seq", flip(bit)) for bit in (1, 2)]
            + [seconds[o - 1][part]]
            for part in range(CORES)
        ]
        for o in offsets
    ]

    lines = -(-(tok // LANES) // 8) * 8
    gain_lines = gain.reshape(full_width // LANES, LANES)

    def norm(core, rows, own, more):
        line = pl.BlockSpec((LANES, feats), lambda b: (b, 0))
        product = pl.BlockSpec((LANES, 2 * head), lambda b: (b, 0))
        sums = pl.BlockSpec((lines, LANES), lambda b: (0, 0))
        return pl.pallas_call(
            norm_kernel,
            grid=(tok // LANES,),
            out_shape=[
                sds((tok, feats), BF16), sds((lines, LANES), F32), sds((tok, 2 * head), F32)
            ],
            in_specs=[SMEM, line, VMEM, VMEM] + ([sums, product] if more else []),
            out_specs=[line, sums, product],
            cost_estimate=pl.CostEstimate(flops=1 << 30, bytes_accessed=1 << 20, transcendentals=0),
            compiler_params=pltpu.CompilerParams(vmem_limit_bytes=40 << 20),
        )((core * (feats // LANES)).reshape(1), rows, gain_lines, own, *more)

    mine, sumsq, acc = norm(h, hidden, own[0], ())
    other, sumsq, acc = norm(h ^ 1, swapped, own[1], (sumsq, acc))
    sqs = [sumsq] + [lax.ppermute(sumsq, "head", shift_x(o)) for o in offsets]

    parts_k, parts_v = [], []
    slabs = jnp.stack([i ^ k for k in range(GROUP)])
    wide, thin = sds((tok, 2 * head), F32), sds((tok, head), BF16)
    for o in offsets:
        half_0, half_1 = blocks[o - 1]
        part = call(early_kernel, wide, [SMEM] + [VMEM] * 4, flops=1 << 29)(
            slabs, mine, other, half_0[0], half_1[0]
        )
        part = call(middle_kernel, wide, [SMEM] + [VMEM] * 5, flops=1 << 29)(
            slabs, mine, part, *half_0[1:]
        )
        part_k, part_v = call(
            late_kernel, [thin, thin], [SMEM] + [VMEM] * 5, flops=1 << 29
        )(slabs, other, part, *half_1[1:])
        parts_k.append(lax.ppermute(part_k, "head", shift_x(o)))
        parts_v.append(lax.ppermute(part_v, "head", shift_x(o)))

    half = head // 2
    freq = 500000.0 ** (-(jnp.arange(half).astype(F32) * 2.0) / head)
    token = s * tok + jnp.arange(tok)
    angle = token.astype(F32)[:, None] * freq[None, :]
    cos, sin = jnp.cos(angle), jnp.sin(angle)
    cos = jnp.concatenate([cos, cos], axis=1)
    sin = jnp.concatenate([-sin, sin], axis=1)

    window = queries.shape[0]
    group_heads = queries.shape[1] // head
    rows = window * group_heads
    row_window = (jnp.arange(rows) % window).astype(jnp.int32)[None, :]
    limit = total_tokens - window + row_window
    expo, stats = call(
        functools.partial(score_kernel, full_width, head ** (-0.5)),
        [sds((tok, rows), F32), sds((n_seq, 2, rows), F32)],
        [SMEM] + [VMEM] * (6 + 2 * len(offsets)),
        scratch=[pltpu.VMEM((tok, head), BF16), pltpu.VMEM((rows, head), BF16)],
        flops=1 << 28,
    )((s * tok).reshape(1), acc, *parts_k, *sqs, cos, sin, queries, limit)
    got = lax.all_to_all(stats, "seq", 0, 0, tiled=True)
    nb = tok // BLK
    vmag = call(
        functools.partial(value_kernel, full_width),
        sds((lines, LANES), F32),
        [VMEM] * (2 + 2 * len(offsets)),
        flops=1 << 28,
    )(acc, *parts_v, *sqs)
    spread = call(
        functools.partial(pool_kernel, window),
        sds((n_seq, LANES), F32),
        [SMEM] + [VMEM] * 5,
        flops=1 << 26,
    )(jnp.concatenate([window_len, kernel_width]), got, stats, expo, vmag, row_window)
    said = lax.all_to_all(spread, "seq", 0, 0, tiled=True)
    local_blocks, fraction = call(
        functools.partial(rank_kernel, nb),
        [sds((1, nb), F32), sds((1, 1), F32)],
        [SMEM, VMEM],
        flops=1 << 20,
    )(jnp.concatenate([kept_block_count, kernel_width, s.reshape(1)]), said)
    return (local_blocks, fraction.reshape(1))


def solution(mesh):
    return jax.shard_map(
        local,
        mesh=mesh,
        in_specs=(
            P("seq", "head"),
            P(),
            P(None, "head"),
            P(None, "head"),
            P(None, "head"),
            P("head"),
            P("head"),
            P("head"),
        ),
        out_specs=(P("head", "seq"), P("head")),
        check_vma=False,
    )
```

```python
import functools

import jax
import jax.numpy as jnp
from jax import lax
from jax.experimental import pallas as pl
from jax.experimental.pallas import tpu as pltpu
from jax.sharding import PartitionSpec as P

BLK = 128
LANES = 128
KERNEL_LIMIT = 15
REACH = (KERNEL_LIMIT - 1) // 2
EDGE = 16
CORES = 2
GROUP = 4
MASKED = -1e30

VMEM = pl.BlockSpec(memory_space=pltpu.VMEM)
SMEM = pl.BlockSpec(memory_space=pltpu.SMEM)
F32, BF16 = jnp.float32, jnp.bfloat16


def sds(shape, dtype):
    return jax.ShapeDtypeStruct(shape, dtype)


def call(body, out, ins, scratch=(), outs=None, flops=1 << 20, limit=40 << 20):
    return pl.pallas_call(
        body,
        out_shape=out,
        in_specs=ins,
        out_specs=outs if outs is not None else jax.tree.map(lambda _: VMEM, out),
        scratch_shapes=list(scratch),
        cost_estimate=pl.CostEstimate(flops=flops, bytes_accessed=1 << 20, transcendentals=0),
        compiler_params=pltpu.CompilerParams(vmem_limit_bytes=limit),
    )


def iota(shape, dim):
    return lax.broadcasted_iota(jnp.int32, shape, dim)


def to_lanes(col):
    n = col.shape[0]
    here = iota((n, LANES), 0) == iota((n, LANES), 1)
    return jnp.sum(jnp.where(here, jnp.broadcast_to(col, (n, LANES)), 0.0), axis=0, keepdims=True)


def to_rows(row, n):
    here = iota((n, LANES), 0) == iota((n, LANES), 1)
    return jnp.sum(jnp.where(here, jnp.broadcast_to(row, (n, LANES)), 0.0), axis=1, keepdims=True)


def norm_kernel(at, hid, gain, weights, *refs):
    more = refs[:-3]
    normed, sumsq, acc = refs[-3:]
    tok, feats = hid.shape
    q = feats // GROUP
    line = at[0]
    sumsq[...] = more[0][...] if more else jnp.zeros_like(sumsq)
    for b in range(tok // LANES):
        rows = pl.ds(b * LANES, LANES)
        folded = None
        for j in range(GROUP):
            place = (at[1] ^ j) * q
            for t in range(q // LANES):
                raw = hid[rows, pl.ds(j * q + t * LANES, LANES)].astype(F32)
                folded = raw * raw if folded is None else folded + raw * raw
                lanes = pl.ds(pl.multiple_of(place + t * LANES, LANES), LANES)
                scale = gain[pl.ds(line + j * (q // LANES) + t, 1), :]
                normed[rows, lanes] = (raw * scale).astype(BF16)
        sumsq[b : b + 1, :] += to_lanes(jnp.sum(folded, axis=1, keepdims=True))
    out = more[1][...] if more else None
    for j in range(GROUP):
        cols = pl.ds(pl.multiple_of((at[1] ^ j) * q, LANES), q)
        p = jnp.dot(normed[:, cols], weights[j * q : (j + 1) * q, :], preferred_element_type=F32)
        out = p if out is None else out + p
    acc[...] = out


def part_of(k, rows, blk):
    q = blk.shape[0]
    return jnp.dot(rows[:, k * q : (k + 1) * q], blk[...], preferred_element_type=F32)


def early_kernel(mine, other, a0, b0, out):
    out[...] = part_of(0, mine, a0) + part_of(0, other, b0)


def middle_kernel(mine, total, a1, a2, a3, out):
    acc = total[...]
    for k, blk in enumerate((a1, a2, a3)):
        acc = acc + part_of(k + 1, mine, blk)
    out[...] = acc


def late_kernel(other, total, b1, b2, b3, out_k, out_v):
    head = out_k.shape[1]
    acc = total[...]
    for k, blk in enumerate((b1, b2, b3)):
        acc = acc + part_of(k + 1, other, blk)
    out_k[...] = acc[:, :head].astype(BF16)
    out_v[...] = acc[:, head:].astype(BF16)


def inverse_rms(sqs, full_width):
    sumsq = sqs[0][...]
    for sq in sqs[1:]:
        sumsq = sumsq + sq[...]
    return lax.rsqrt(sumsq / full_width + 1e-05)


def score_kernel(full_width, scale_by, *refs):
    n_off = (len(refs) - 10) // 2
    acc, parts, sqs = refs[0], refs[1 : 1 + n_off], refs[1 + n_off : 2 + 2 * n_off]
    cos, sin, q, room, expo, stats, keys, rows_of = refs[2 + 2 * n_off :]
    tok, head = keys.shape
    window = q.shape[0]
    for j in range(q.shape[1] // head):
        rows_of[j * window : (j + 1) * window, :] = q[:, j * head : (j + 1) * head]
    inv = inverse_rms(sqs, full_width)
    for b in range(tok // LANES):
        rows = pl.ds(b * LANES, LANES)
        k = acc[rows, :head]
        for p in parts:
            k = k + p[rows, :].astype(F32)
        k = k * to_rows(inv[b : b + 1, :], LANES)
        keys[rows, :] = (k * cos[rows, :] + pltpu.roll(k, head // 2, 1) * sin[rows, :]).astype(BF16)
    scores = lax.dot_general(
        keys[...], rows_of[...], (((1,), (1,)), ((), ())), preferred_element_type=F32
    ) * scale_by
    open_to = tok - window
    tail = jnp.where(iota((window, 1), 0) <= room[...], scores[open_to:, :], MASKED)
    body = scores[:open_to, :]
    top = jnp.maximum(
        jnp.max(body, axis=0, keepdims=True), jnp.max(tail, axis=0, keepdims=True)
    )
    body, tail = jnp.exp(body - top), jnp.exp(tail - top)
    expo[:open_to, :] = body
    expo[open_to:, :] = tail
    own = jnp.sum(body, axis=0, keepdims=True) + jnp.sum(tail, axis=0, keepdims=True)
    for d in range(stats.shape[0]):
        stats[d, 0:1, :] = top
        stats[d, 1:2, :] = own


def value_kernel(full_width, *refs):
    n_off = (len(refs) - 3) // 2
    acc, parts, sqs, out = refs[0], refs[1 : 1 + n_off], refs[1 + n_off : 2 + 2 * n_off], refs[-1]
    head = acc.shape[1] // 2
    inv = inverse_rms(sqs, full_width)
    out[...] = jnp.zeros_like(out)
    for b in range(acc.shape[0] // LANES):
        rows = pl.ds(b * LANES, LANES)
        v = acc[rows, head:]
        for p in parts:
            v = v + p[rows, :].astype(F32)
        total = to_lanes(jnp.sum(jnp.abs(v), axis=1, keepdims=True))
        out[b : b + 1, :] = total * (1.0 / head) * inv[b : b + 1, :]


def widen(column, below, above, lane, halfspan):
    pooled = column
    for shift in range(1, REACH + 1):
        right = pltpu.roll(jnp.where(lane < shift, below, column), LANES - shift, 1)
        left = pltpu.roll(jnp.where(lane >= LANES - shift, above, column), shift, 1)
        pooled = jnp.where(
            shift <= halfspan, jnp.maximum(jnp.maximum(pooled, right), left), pooled
        )
    return pooled


def pool_kernel(reach, got, mine, expo, vmag, used, spread):
    tok = expo.shape[0]
    nb = tok // LANES
    row_top = got[0, 0:1, :]
    for d in range(1, got.shape[0]):
        row_top = jnp.maximum(row_top, got[d, 0:1, :])
    row_total = jnp.zeros_like(row_top)
    for d in range(got.shape[0]):
        row_total = row_total + got[d, 1:2, :] * jnp.exp(got[d, 0:1, :] - row_top)
    weight = used[...] * jnp.exp(mine[0, 0:1, :] - row_top) / row_total
    height = vmag.shape[0]
    line = iota((height, LANES), 0)
    lane = iota((height, LANES), 1)
    column = jnp.zeros((height, LANES), F32)
    for b in range(nb):
        mass = jnp.sum(expo[b * LANES : (b + 1) * LANES, :] * weight, axis=1, keepdims=True)
        column = jnp.where(line == b, jnp.broadcast_to(to_lanes(mass), (height, LANES)), column)
    column = column * vmag[...]
    below, above = pltpu.roll(column, height - 1, 0), pltpu.roll(column, 1, 0)
    pooled = widen(column, below, above, lane, reach[...])
    place = line * LANES + lane
    inner = (place >= REACH) & (place < tok - REACH)
    sums = to_lanes(jnp.sum(jnp.where(inner, pooled, 0.0), axis=1, keepdims=True))
    flat = lane[0:1, :]
    last = pltpu.roll(column[nb - 1 : nb, :], 2 * EDGE, 1)
    said = jnp.where(flat < EDGE, column[0:1, :], jnp.where(flat < 2 * EDGE, last, pltpu.roll(sums, 2 * EDGE, 1)))
    spread[...] = jnp.broadcast_to(said, spread.shape)


def rank_kernel(nb, keep, reach, here, said, blocks, share):
    v = said[...]
    n = v.shape[0]
    line, lane = iota(v.shape, 0), iota(v.shape, 1)
    following = pltpu.roll(v, n - 1, 0)
    seam = jnp.where(lane < EDGE, pltpu.roll(v, LANES - EDGE, 1), pltpu.roll(following, EDGE, 1))
    seam = jnp.where(lane < 2 * EDGE, seam, 0.0)
    end = line == n - 1
    apart = LANES // 2
    both = jnp.where(end & (lane >= EDGE), 0.0, seam) + pltpu.roll(
        jnp.where(end & (lane < EDGE), 0.0, seam), apart, 1
    )
    pooled = both
    for shift in range(1, REACH + 1):
        near = jnp.maximum(pltpu.roll(both, shift, 1), pltpu.roll(both, LANES - shift, 1))
        pooled = jnp.where(shift <= reach[...], jnp.maximum(pooled, near), pooled)
    tail = (lane >= EDGE - REACH) & (lane < EDGE)
    lead = (lane >= apart + EDGE) & (lane < apart + EDGE + REACH)
    tail = jnp.sum(jnp.where(tail, pooled, 0.0), axis=1, keepdims=True)
    lead = jnp.sum(jnp.where(lead, pooled, 0.0), axis=1, keepdims=True)
    lead = pltpu.roll(jnp.broadcast_to(lead, v.shape), 1, 0)
    b = pltpu.roll(v, LANES - 2 * EDGE, 1)
    b = b + jnp.where(lane == 0, lead, 0.0) + jnp.where(lane == nb - 1, tail, 0.0)
    b = jnp.where(lane < nb, b, 0.0)
    own = jnp.sum(jnp.where(line == here[...], b, 0.0), axis=0, keepdims=True)
    blocks[...] = own[:, :nb]
    place = line * nb + lane
    rank = jnp.zeros(v.shape, jnp.int32)

    def turned(t, k):
        return jnp.where(lane >= k, pltpu.roll(t, k, 1), pltpu.roll(t, LANES + k - nb, 1)) if k else t

    for k in range(nb):
        bk, pk = turned(b, k), turned(place, k)
        for m in range(n):
            bm, pm = (pltpu.roll(bk, m, 0), pltpu.roll(pk, m, 0)) if m else (bk, pk)
            rank = rank + jnp.where((bm > b) | ((bm == b) & (pm < place)), 1, 0)

    def add(t):
        return jnp.sum(jnp.sum(t, axis=1, keepdims=True), axis=0, keepdims=True)

    kept = jnp.where((lane < nb) & (rank < keep[...]), b, 0.0)
    share[...] = add(kept) / add(b)


def local(
    hidden, gain, key_matrix, value_matrix, queries, window_len, kernel_width, kept_block_count
):
    tok, feats = hidden.shape
    full_width = gain.shape[0]
    head = key_matrix.shape[1]
    n_seq, n_head = lax.axis_size("seq"), lax.axis_size("head")
    n_x = n_head // CORES
    s, h = lax.axis_index("seq"), lax.axis_index("head")
    x, c = h // CORES, h % CORES
    i = s % GROUP
    q = feats // GROUP
    total_tokens = tok * n_seq
    offsets = range(1, n_x)

    def shift_x(offset):
        return [
            (a * CORES + b, (a + offset) % n_x * CORES + b) for a in range(n_x) for b in range(CORES)
        ]

    def flip(bit):
        return [(j, j ^ bit) for j in range(n_seq)]

    def rows_at(start, count):
        return jnp.concatenate(
            [lax.dynamic_slice_in_dim(m, start, count) for m in (key_matrix, value_matrix)], axis=1
        )

    def crossing(block):
        return [
            [
                rows_at(((x - o) % n_x * CORES + (c ^ part)) * feats + block * q, q)
                for part in range(CORES)
            ]
            for o in offsets
        ]

    def cross(rows):
        return [
            [lax.ppermute(rows[o - 1][part], "head", shift_x(-o)) for part in range(CORES)]
            for o in offsets
        ]

    lead = crossing(i)
    lead[0][0], key_matrix, value_matrix = lax.optimization_barrier(
        (lead[0][0], key_matrix, value_matrix)
    )
    firsts = cross([lead[0][:1] + rest[1:] if k == 0 else rest for k, rest in enumerate(crossing(i))])
    seconds = cross(crossing(3 - i))
    own = [rows_at(start * feats, feats) for start in (h, h ^ 1)]
    swapped = lax.ppermute(hidden, "head", [(j, j ^ 1) for j in range(n_head)])
    blocks = [
        [
            [firsts[o - 1][part]]
            + [lax.ppermute(firsts[o - 1][part], "seq", flip(bit)) for bit in (1, 2)]
            + [seconds[o - 1][part]]
            for part in range(CORES)
        ]
        for o in offsets
    ]

    lines = -(-(tok // LANES) // 8) * 8
    gain_lines = gain.reshape(full_width // LANES, LANES)

    def norm(core, rows, own, more):
        return call(
            norm_kernel,
            [sds((tok, feats), BF16), sds((lines, LANES), F32), sds((tok, 2 * head), F32)],
            [SMEM] + [VMEM] * (3 + len(more)),
            flops=1 << 30,
        )(jnp.stack([core * (feats // LANES), i]), rows, gain_lines, own, *more)

    mine, sumsq, acc = norm(h, hidden, own[0], ())

    window = queries.shape[0]
    group_heads = queries.shape[1] // head
    rows = window * group_heads
    row_window = (jnp.arange(rows) % window).astype(jnp.int32)[None, :]
    room = total_tokens - window + row_window - (s * tok + tok - window)
    used = (row_window >= window - window_len[0]).astype(F32)
    reach = jnp.broadcast_to((kernel_width - 1) // 2, (1, LANES))
    keep = jnp.broadcast_to(kept_block_count, (1, LANES))
    here = jnp.broadcast_to(s, (1, LANES)).astype(jnp.int32)
    swapped, room, used, reach = lax.optimization_barrier((swapped, room, used, reach))
    other, sumsq, acc = norm(h ^ 1, swapped, own[1], (sumsq, acc))
    sqs = [sumsq] + [lax.ppermute(sumsq, "head", shift_x(o)) for o in offsets]

    parts_k, parts_v = [], []
    wide, thin = sds((tok, 2 * head), F32), sds((tok, head), BF16)
    for o in offsets:
        half_0, half_1 = blocks[o - 1]
        part = call(early_kernel, wide, [VMEM] * 4, flops=1 << 29)(
            mine, other, half_0[0], half_1[0]
        )
        part = call(middle_kernel, wide, [VMEM] * 5, flops=1 << 29)(mine, part, *half_0[1:])
        part_k, part_v = call(
            late_kernel, [thin, thin], [VMEM] * 5, flops=1 << 29
        )(other, part, *half_1[1:])
        parts_k.append(lax.ppermute(part_k, "head", shift_x(o)))
        parts_v.append(lax.ppermute(part_v, "head", shift_x(o)))

    half = head // 2
    freq = 500000.0 ** (-(jnp.arange(half).astype(F32) * 2.0) / head)
    token = s * tok + jnp.arange(tok)
    angle = token.astype(F32)[:, None] * freq[None, :]
    cos, sin = jnp.cos(angle), jnp.sin(angle)
    cos = jnp.concatenate([cos, cos], axis=1)
    sin = jnp.concatenate([-sin, sin], axis=1)

    expo, stats = call(
        functools.partial(score_kernel, full_width, head ** (-0.5)),
        [sds((tok, rows), F32), sds((n_seq, 2, rows), F32)],
        [VMEM] * (6 + 2 * len(offsets)),
        scratch=[pltpu.VMEM((tok, head), BF16), pltpu.VMEM((rows, head), BF16)],
        flops=1 << 28,
    )(acc, *parts_k, *sqs, cos, sin, queries, room)
    got = lax.all_to_all(stats, "seq", 0, 0, tiled=True)
    nb = tok // BLK
    vmag = call(
        functools.partial(value_kernel, full_width),
        sds((lines, LANES), F32),
        [VMEM] * (2 + 2 * len(offsets)),
        flops=1 << 28,
    )(acc, *parts_v, *sqs)
    spread = call(
        pool_kernel, sds((n_seq, LANES), F32), [VMEM] * 6, flops=1 << 26
    )(reach, got, stats, expo, vmag, used)
    said = lax.all_to_all(spread, "seq", 0, 0, tiled=True)
    local_blocks, fraction = call(
        functools.partial(rank_kernel, nb),
        [sds((1, nb), F32), sds((1, 1), F32)],
        [VMEM] * 4,
        flops=1 << 20,
    )(keep, reach, here, said)
    return (local_blocks, fraction.reshape(1))


def solution(mesh):
    return jax.shard_map(
        local,
        mesh=mesh,
        in_specs=(
            P("seq", "head"),
            P(),
            P(None, "head"),
            P(None, "head"),
            P(None, "head"),
            P("head"),
            P("head"),
            P("head"),
        ),
        out_specs=(P("head", "seq"), P("head")),
        check_vma=False,
    )
```

```python
import functools

import jax
import jax.numpy as jnp
from jax import lax
from jax.experimental import pallas as pl
from jax.experimental.pallas import tpu as pltpu
from jax.sharding import PartitionSpec as P

BLK = 128
LANES = 128
KERNEL_LIMIT = 15
REACH = (KERNEL_LIMIT - 1) // 2
EDGE = 16
CORES = 2
GROUP = 4
MASKED = -1e30

VMEM = pl.BlockSpec(memory_space=pltpu.VMEM)
SMEM = pl.BlockSpec(memory_space=pltpu.SMEM)
F32, BF16 = jnp.float32, jnp.bfloat16


def sds(shape, dtype):
    return jax.ShapeDtypeStruct(shape, dtype)


def call(body, out, ins, scratch=(), outs=None, flops=1 << 20, limit=40 << 20):
    return pl.pallas_call(
        body,
        out_shape=out,
        in_specs=ins,
        out_specs=outs if outs is not None else jax.tree.map(lambda _: VMEM, out),
        scratch_shapes=list(scratch),
        cost_estimate=pl.CostEstimate(flops=flops, bytes_accessed=1 << 20, transcendentals=0),
        compiler_params=pltpu.CompilerParams(vmem_limit_bytes=limit),
    )


def iota(shape, dim):
    return lax.broadcasted_iota(jnp.int32, shape, dim)


def to_lanes(col):
    n = col.shape[0]
    here = iota((n, LANES), 0) == iota((n, LANES), 1)
    return jnp.sum(jnp.where(here, jnp.broadcast_to(col, (n, LANES)), 0.0), axis=0, keepdims=True)


def to_rows(row, n):
    here = iota((n, LANES), 0) == iota((n, LANES), 1)
    return jnp.sum(jnp.where(here, jnp.broadcast_to(row, (n, LANES)), 0.0), axis=1, keepdims=True)


def norm_kernel(at, hid, gain, weights, *refs):
    more = refs[:-3]
    normed, sumsq, acc = refs[-3:]
    tok, feats = hid.shape
    q = feats // GROUP
    line = at[0]
    sumsq[...] = more[0][...] if more else jnp.zeros_like(sumsq)
    for b in range(tok // LANES):
        rows = pl.ds(b * LANES, LANES)
        folded = None
        for j in range(GROUP):
            place = (at[1] ^ j) * q
            for t in range(q // LANES):
                raw = hid[rows, pl.ds(j * q + t * LANES, LANES)].astype(F32)
                folded = raw * raw if folded is None else folded + raw * raw
                lanes = pl.ds(pl.multiple_of(place + t * LANES, LANES), LANES)
                scale = gain[pl.ds(line + j * (q // LANES) + t, 1), :]
                normed[rows, lanes] = (raw * scale).astype(BF16)
        sumsq[b : b + 1, :] += to_lanes(jnp.sum(folded, axis=1, keepdims=True))
    out = more[1][...] if more else None
    for j in range(GROUP):
        cols = pl.ds(pl.multiple_of((at[1] ^ j) * q, LANES), q)
        p = jnp.dot(normed[:, cols], weights[j * q : (j + 1) * q, :], preferred_element_type=F32)
        out = p if out is None else out + p
    acc[...] = out


def part_of(k, rows, blk):
    q = blk.shape[0]
    return jnp.dot(rows[:, k * q : (k + 1) * q], blk[...], preferred_element_type=F32)


def early_kernel(mine, other, a0, b0, out):
    out[...] = part_of(0, mine, a0) + part_of(0, other, b0)


def middle_kernel(mine, total, a1, a2, a3, out):
    acc = total[...]
    for k, blk in enumerate((a1, a2, a3)):
        acc = acc + part_of(k + 1, mine, blk)
    out[...] = acc


def late_kernel(other, total, b1, b2, b3, out_k, out_v):
    head = out_k.shape[1]
    acc = total[...]
    for k, blk in enumerate((b1, b2, b3)):
        acc = acc + part_of(k + 1, other, blk)
    out_k[...] = acc[:, :head].astype(BF16)
    out_v[...] = acc[:, head:].astype(BF16)


def inverse_rms(sqs, full_width):
    sumsq = sqs[0][...]
    for sq in sqs[1:]:
        sumsq = sumsq + sq[...]
    return lax.rsqrt(sumsq / full_width + 1e-05)


def score_kernel(full_width, scale_by, *refs):
    n_off = (len(refs) - 10) // 2
    acc, parts, sqs = refs[0], refs[1 : 1 + n_off], refs[1 + n_off : 2 + 2 * n_off]
    cos, sin, q, room, expo, stats, keys, rows_of = refs[2 + 2 * n_off :]
    tok, head = keys.shape
    window = q.shape[0]
    for j in range(q.shape[1] // head):
        rows_of[j * window : (j + 1) * window, :] = q[:, j * head : (j + 1) * head]
    inv = inverse_rms(sqs, full_width)
    for b in range(tok // LANES):
        rows = pl.ds(b * LANES, LANES)
        k = acc[rows, :head]
        for p in parts:
            k = k + p[rows, :].astype(F32)
        k = k * to_rows(inv[b : b + 1, :], LANES)
        keys[rows, :] = (k * cos[rows, :] + pltpu.roll(k, head // 2, 1) * sin[rows, :]).astype(BF16)
    scores = lax.dot_general(
        keys[...], rows_of[...], (((1,), (1,)), ((), ())), preferred_element_type=F32
    ) * scale_by
    open_to = tok - window
    tail = jnp.where(iota((window, 1), 0) <= room[...], scores[open_to:, :], MASKED)
    body = scores[:open_to, :]
    top = jnp.maximum(
        jnp.max(body, axis=0, keepdims=True), jnp.max(tail, axis=0, keepdims=True)
    )
    body, tail = jnp.exp(body - top), jnp.exp(tail - top)
    expo[:open_to, :] = body
    expo[open_to:, :] = tail
    own = jnp.sum(body, axis=0, keepdims=True) + jnp.sum(tail, axis=0, keepdims=True)
    for d in range(stats.shape[0]):
        stats[d, 0:1, :] = top
        stats[d, 1:2, :] = own


def value_kernel(full_width, *refs):
    n_off = (len(refs) - 3) // 2
    acc, parts, sqs, out = refs[0], refs[1 : 1 + n_off], refs[1 + n_off : 2 + 2 * n_off], refs[-1]
    head = acc.shape[1] // 2
    inv = inverse_rms(sqs, full_width)
    out[...] = jnp.zeros_like(out)
    for b in range(acc.shape[0] // LANES):
        rows = pl.ds(b * LANES, LANES)
        v = acc[rows, head:]
        for p in parts:
            v = v + p[rows, :].astype(F32)
        total = to_lanes(jnp.sum(jnp.abs(v), axis=1, keepdims=True))
        out[b : b + 1, :] = total * (1.0 / head) * inv[b : b + 1, :]


def widen(column, below, above, lane, halfspan):
    pooled = column
    for shift in range(1, REACH + 1):
        right = pltpu.roll(jnp.where(lane < shift, below, column), LANES - shift, 1)
        left = pltpu.roll(jnp.where(lane >= LANES - shift, above, column), shift, 1)
        pooled = jnp.where(
            shift <= halfspan, jnp.maximum(jnp.maximum(pooled, right), left), pooled
        )
    return pooled


def pool_kernel(reach, got, mine, expo, vmag, used, spread):
    tok = expo.shape[0]
    nb = tok // LANES
    row_top = got[0, 0:1, :]
    for d in range(1, got.shape[0]):
        row_top = jnp.maximum(row_top, got[d, 0:1, :])
    row_total = jnp.zeros_like(row_top)
    for d in range(got.shape[0]):
        row_total = row_total + got[d, 1:2, :] * jnp.exp(got[d, 0:1, :] - row_top)
    weight = used[...] * jnp.exp(mine[0, 0:1, :] - row_top) / row_total
    height = vmag.shape[0]
    line = iota((height, LANES), 0)
    lane = iota((height, LANES), 1)
    column = jnp.zeros((height, LANES), F32)
    for b in range(nb):
        mass = jnp.sum(expo[b * LANES : (b + 1) * LANES, :] * weight, axis=1, keepdims=True)
        column = jnp.where(line == b, jnp.broadcast_to(to_lanes(mass), (height, LANES)), column)
    column = column * vmag[...]
    below, above = pltpu.roll(column, height - 1, 0), pltpu.roll(column, 1, 0)
    pooled = widen(column, below, above, lane, reach[...])
    place = line * LANES + lane
    inner = (place >= REACH) & (place < tok - REACH)
    sums = to_lanes(jnp.sum(jnp.where(inner, pooled, 0.0), axis=1, keepdims=True))
    flat = lane[0:1, :]
    last = pltpu.roll(column[nb - 1 : nb, :], 2 * EDGE, 1)
    said = jnp.where(flat < EDGE, column[0:1, :], jnp.where(flat < 2 * EDGE, last, pltpu.roll(sums, 2 * EDGE, 1)))
    spread[...] = jnp.broadcast_to(said, spread.shape)


def rank_kernel(nb, keep, reach, here, said, blocks, share):
    v = said[...]
    n = v.shape[0]
    line, lane = iota(v.shape, 0), iota(v.shape, 1)
    following = pltpu.roll(v, n - 1, 0)
    seam = jnp.where(lane < EDGE, pltpu.roll(v, LANES - EDGE, 1), pltpu.roll(following, EDGE, 1))
    seam = jnp.where(lane < 2 * EDGE, seam, 0.0)
    end = line == n - 1
    apart = LANES // 2
    both = jnp.where(end & (lane >= EDGE), 0.0, seam) + pltpu.roll(
        jnp.where(end & (lane < EDGE), 0.0, seam), apart, 1
    )
    pooled = both
    for shift in range(1, REACH + 1):
        near = jnp.maximum(pltpu.roll(both, shift, 1), pltpu.roll(both, LANES - shift, 1))
        pooled = jnp.where(shift <= reach[...], jnp.maximum(pooled, near), pooled)
    tail = (lane >= EDGE - REACH) & (lane < EDGE)
    lead = (lane >= apart + EDGE) & (lane < apart + EDGE + REACH)
    tail = jnp.sum(jnp.where(tail, pooled, 0.0), axis=1, keepdims=True)
    lead = jnp.sum(jnp.where(lead, pooled, 0.0), axis=1, keepdims=True)
    lead = pltpu.roll(jnp.broadcast_to(lead, v.shape), 1, 0)
    b = pltpu.roll(v, LANES - 2 * EDGE, 1)
    b = b + jnp.where(lane == 0, lead, 0.0) + jnp.where(lane == nb - 1, tail, 0.0)
    b = jnp.where(lane < nb, b, 0.0)
    own = jnp.sum(jnp.where(line == here[...], b, 0.0), axis=0, keepdims=True)
    blocks[...] = own[:, :nb]
    place = line * nb + lane
    rank = jnp.zeros(v.shape, jnp.int32)

    def turned(t, k):
        return jnp.where(lane >= k, pltpu.roll(t, k, 1), pltpu.roll(t, LANES + k - nb, 1)) if k else t

    for k in range(nb):
        bk, pk = turned(b, k), turned(place, k)
        for m in range(n):
            bm, pm = (pltpu.roll(bk, m, 0), pltpu.roll(pk, m, 0)) if m else (bk, pk)
            rank = rank + jnp.where((bm > b) | ((bm == b) & (pm < place)), 1, 0)

    def add(t):
        return jnp.sum(jnp.sum(t, axis=1, keepdims=True), axis=0, keepdims=True)

    kept = jnp.where((lane < nb) & (rank < keep[...]), b, 0.0)
    share[...] = add(kept) / add(b)


def local(
    hidden, gain, key_matrix, value_matrix, queries, window_len, kernel_width, kept_block_count
):
    tok, feats = hidden.shape
    full_width = gain.shape[0]
    head = key_matrix.shape[1]
    n_seq, n_head = lax.axis_size("seq"), lax.axis_size("head")
    n_x = n_head // CORES
    s, h = lax.axis_index("seq"), lax.axis_index("head")
    x, c = h // CORES, h % CORES
    i = s % GROUP
    q = feats // GROUP
    total_tokens = tok * n_seq
    offsets = range(1, n_x)

    def shift_x(offset, cores=range(CORES)):
        return [(a * CORES + b, (a + offset) % n_x * CORES + b) for a in range(n_x) for b in cores]

    def flip(bit):
        return [(j, j ^ bit) for j in range(n_seq)]

    def rows_at(start, count):
        return jnp.concatenate(
            [lax.dynamic_slice_in_dim(m, start, count) for m in (key_matrix, value_matrix)], axis=1
        )

    def crossing(block):
        return [
            [
                rows_at(((x - o) % n_x * CORES + (c ^ part)) * feats + block * q, q)
                for part in range(CORES)
            ]
            for o in offsets
        ]

    def piece(name, part, o, rows, following):
        if name != "first" or part:
            return lax.ppermute(rows, "head", shift_x(-o))
        later, following[1] = lax.optimization_barrier((rows, following[1]))
        ahead = lax.ppermute(rows, "head", shift_x(-o, (0,)))
        behind = lax.ppermute(later, "head", shift_x(-o, (1,)))
        return jnp.where(c == 0, ahead, behind)

    def cross(name, rows):
        return [
            [piece(name, part, o, rows[o - 1][part], rows[o - 1]) for part in range(CORES)]
            for o in offsets
        ]

    lead = crossing(i)
    lead[0][0], key_matrix, value_matrix = lax.optimization_barrier(
        (lead[0][0], key_matrix, value_matrix)
    )
    firsts = cross("first", [lead[0][:1] + rest[1:] if k == 0 else rest for k, rest in enumerate(crossing(i))])
    seconds = cross("second", crossing(3 - i))
    own = [rows_at(start * feats, feats) for start in (h, h ^ 1)]
    swapped = lax.ppermute(hidden, "head", [(j, j ^ 1) for j in range(n_head)])
    blocks = [
        [
            [firsts[o - 1][part]]
            + [lax.ppermute(firsts[o - 1][part], "seq", flip(bit)) for bit in (1, 2)]
            + [seconds[o - 1][part]]
            for part in range(CORES)
        ]
        for o in offsets
    ]

    lines = -(-(tok // LANES) // 8) * 8
    gain_lines = gain.reshape(full_width // LANES, LANES)

    def norm(core, rows, own, more):
        return call(
            norm_kernel,
            [sds((tok, feats), BF16), sds((lines, LANES), F32), sds((tok, 2 * head), F32)],
            [SMEM] + [VMEM] * (3 + len(more)),
            flops=1 << 30,
        )(jnp.stack([core * (feats // LANES), i]), rows, gain_lines, own, *more)

    mine, sumsq, acc = norm(h, hidden, own[0], ())

    window = queries.shape[0]
    group_heads = queries.shape[1] // head
    rows = window * group_heads
    row_window = (jnp.arange(rows) % window).astype(jnp.int32)[None, :]
    room = total_tokens - window + row_window - (s * tok + tok - window)
    used = (row_window >= window - window_len[0]).astype(F32)
    reach = jnp.broadcast_to((kernel_width - 1) // 2, (1, LANES))
    keep = jnp.broadcast_to(kept_block_count, (1, LANES))
    here = jnp.broadcast_to(s, (1, LANES)).astype(jnp.int32)
    swapped, room, used, reach, keep, here = lax.optimization_barrier(
        (swapped, room, used, reach, keep, here)
    )
    other, sumsq, acc = norm(h ^ 1, swapped, own[1], (sumsq, acc))
    sqs = [sumsq] + [lax.ppermute(sumsq, "head", shift_x(o)) for o in offsets]

    parts_k, parts_v = [], []
    wide, thin = sds((tok, 2 * head), F32), sds((tok, head), BF16)
    for o in offsets:
        half_0, half_1 = blocks[o - 1]
        part = call(early_kernel, wide, [VMEM] * 4, flops=1 << 29)(
            mine, other, half_0[0], half_1[0]
        )
        part = call(middle_kernel, wide, [VMEM] * 5, flops=1 << 29)(mine, part, *half_0[1:])
        part_k, part_v = call(
            late_kernel, [thin, thin], [VMEM] * 5, flops=1 << 29
        )(other, part, *half_1[1:])
        parts_k.append(lax.ppermute(part_k, "head", shift_x(o)))
        parts_v.append(lax.ppermute(part_v, "head", shift_x(o)))

    half = head // 2
    freq = 500000.0 ** (-(jnp.arange(half).astype(F32) * 2.0) / head)
    token = s * tok + jnp.arange(tok)
    angle = token.astype(F32)[:, None] * freq[None, :]
    cos, sin = jnp.cos(angle), jnp.sin(angle)
    cos = jnp.concatenate([cos, cos], axis=1)
    sin = jnp.concatenate([-sin, sin], axis=1)

    expo, stats = call(
        functools.partial(score_kernel, full_width, head ** (-0.5)),
        [sds((tok, rows), F32), sds((n_seq, 2, rows), F32)],
        [VMEM] * (6 + 2 * len(offsets)),
        scratch=[pltpu.VMEM((tok, head), BF16), pltpu.VMEM((rows, head), BF16)],
        flops=1 << 28,
    )(acc, *parts_k, *sqs, cos, sin, queries, room)
    got = lax.all_to_all(stats, "seq", 0, 0, tiled=True)
    nb = tok // BLK
    vmag = call(
        functools.partial(value_kernel, full_width),
        sds((lines, LANES), F32),
        [VMEM] * (2 + 2 * len(offsets)),
        flops=1 << 28,
    )(acc, *parts_v, *sqs)
    spread = call(
        pool_kernel, sds((n_seq, LANES), F32), [VMEM] * 6, flops=1 << 26
    )(reach, got, stats, expo, vmag, used)
    said = lax.all_to_all(spread, "seq", 0, 0, tiled=True)
    local_blocks, fraction = call(
        functools.partial(rank_kernel, nb),
        [sds((1, nb), F32), sds((1, 1), F32)],
        [VMEM] * 4,
        flops=1 << 20,
    )(keep, reach, here, said)
    return (local_blocks, fraction.reshape(1))


def solution(mesh):
    return jax.shard_map(
        local,
        mesh=mesh,
        in_specs=(
            P("seq", "head"),
            P(),
            P(None, "head"),
            P(None, "head"),
            P(None, "head"),
            P("head"),
            P("head"),
            P("head"),
        ),
        out_specs=(P("head", "seq"), P("head")),
        check_vma=False,
    )
```

```python
import functools

import jax
import jax.numpy as jnp
from jax import lax
from jax.experimental import pallas as pl
from jax.experimental.pallas import tpu as pltpu
from jax.sharding import PartitionSpec as P

BLK = 128
LANES = 128
KERNEL_LIMIT = 15
REACH = (KERNEL_LIMIT - 1) // 2
EDGE = 16
CORES = 2
GROUP = 4
MASKED = -1e30

VMEM = pl.BlockSpec(memory_space=pltpu.VMEM)
SMEM = pl.BlockSpec(memory_space=pltpu.SMEM)
F32, BF16 = jnp.float32, jnp.bfloat16


def sds(shape, dtype):
    return jax.ShapeDtypeStruct(shape, dtype)


def call(body, out, ins, scratch=(), outs=None, flops=1 << 20, limit=40 << 20):
    return pl.pallas_call(
        body,
        out_shape=out,
        in_specs=ins,
        out_specs=outs if outs is not None else jax.tree.map(lambda _: VMEM, out),
        scratch_shapes=list(scratch),
        cost_estimate=pl.CostEstimate(flops=flops, bytes_accessed=1 << 20, transcendentals=0),
        compiler_params=pltpu.CompilerParams(vmem_limit_bytes=limit),
    )


def iota(shape, dim):
    return lax.broadcasted_iota(jnp.int32, shape, dim)


def to_lanes(col):
    n = col.shape[0]
    here = iota((n, LANES), 0) == iota((n, LANES), 1)
    return jnp.sum(jnp.where(here, jnp.broadcast_to(col, (n, LANES)), 0.0), axis=0, keepdims=True)


def to_rows(row, n):
    here = iota((n, LANES), 0) == iota((n, LANES), 1)
    return jnp.sum(jnp.where(here, jnp.broadcast_to(row, (n, LANES)), 0.0), axis=1, keepdims=True)


def norm_kernel(at, hid, gain, keys, values, *refs):
    more = refs[:-3]
    normed, sumsq, acc = refs[-3:]
    tok, feats = hid.shape
    q = feats // GROUP
    line = at[0]
    sumsq[...] = more[0][...] if more else jnp.zeros_like(sumsq)
    for b in range(tok // LANES):
        rows = pl.ds(b * LANES, LANES)
        folded = None
        for j in range(GROUP):
            place = (at[1] ^ j) * q
            for t in range(q // LANES):
                raw = hid[rows, pl.ds(j * q + t * LANES, LANES)].astype(F32)
                folded = raw * raw if folded is None else folded + raw * raw
                lanes = pl.ds(pl.multiple_of(place + t * LANES, LANES), LANES)
                scale = gain[pl.ds(line + j * (q // LANES) + t, 1), :]
                normed[rows, lanes] = (raw * scale).astype(BF16)
        sumsq[b : b + 1, :] += to_lanes(jnp.sum(folded, axis=1, keepdims=True))
    blocks = [
        jnp.concatenate(
            [w[pl.ds(pl.multiple_of((at[1] ^ k) * q, LANES), q), :] for k in range(GROUP)], axis=0
        )
        for w in (keys, values)
    ]
    out = jnp.dot(
        normed[...], jnp.concatenate(blocks, axis=1), preferred_element_type=F32
    )
    acc[...] = out + more[1][...] if more else out


def part_of(rows, blks):
    weights = [jnp.concatenate([b[...] for b in blks[side::2]], axis=0) for side in range(2)]
    return jnp.dot(rows, jnp.concatenate(weights, axis=1), preferred_element_type=F32)


def early_kernel(mine, other, a_k, a_v, b_k, b_v, out):
    q = a_k.shape[0]
    out[...] = part_of(mine[:, :q], (a_k, a_v)) + part_of(other[:, :q], (b_k, b_v))


def middle_kernel(mine, total, *refs):
    blks, out = refs[:-1], refs[-1]
    out[...] = total[...] + part_of(mine[:, blks[0].shape[0] :], blks)


def late_kernel(other, total, *refs):
    blks, out_k, out_v = refs[:-2], refs[-2], refs[-1]
    head = out_k.shape[1]
    acc = total[...] + part_of(other[:, blks[0].shape[0] :], blks)
    out_k[...] = acc[:, :head].astype(BF16)
    out_v[...] = acc[:, head:].astype(BF16)


def inverse_rms(sqs, full_width):
    sumsq = sqs[0][...]
    for sq in sqs[1:]:
        sumsq = sumsq + sq[...]
    return lax.rsqrt(sumsq / full_width + 1e-05)


def score_kernel(full_width, scale_by, *refs):
    n_off = (len(refs) - 10) // 2
    acc, parts, sqs = refs[0], refs[1 : 1 + n_off], refs[1 + n_off : 2 + 2 * n_off]
    cos, sin, q, room, expo, stats, keys, rows_of = refs[2 + 2 * n_off :]
    tok, head = keys.shape
    window = q.shape[0]
    for j in range(q.shape[1] // head):
        rows_of[j * window : (j + 1) * window, :] = q[:, j * head : (j + 1) * head]
    inv = inverse_rms(sqs, full_width)
    for b in range(tok // LANES):
        rows = pl.ds(b * LANES, LANES)
        k = acc[rows, :head]
        for p in parts:
            k = k + p[rows, :].astype(F32)
        k = k * to_rows(inv[b : b + 1, :], LANES)
        keys[rows, :] = (k * cos[rows, :] + pltpu.roll(k, head // 2, 1) * sin[rows, :]).astype(BF16)
    scores = lax.dot_general(
        keys[...], rows_of[...], (((1,), (1,)), ((), ())), preferred_element_type=F32
    ) * scale_by
    open_to = tok - window
    tail = jnp.where(iota((window, 1), 0) <= room[...], scores[open_to:, :], MASKED)
    body = scores[:open_to, :]
    top = jnp.maximum(
        jnp.max(body, axis=0, keepdims=True), jnp.max(tail, axis=0, keepdims=True)
    )
    body, tail = jnp.exp(body - top), jnp.exp(tail - top)
    expo[:open_to, :] = body
    expo[open_to:, :] = tail
    own = jnp.sum(body, axis=0, keepdims=True) + jnp.sum(tail, axis=0, keepdims=True)
    for d in range(stats.shape[0]):
        stats[d, 0:1, :] = top
        stats[d, 1:2, :] = own


def value_kernel(full_width, *refs):
    n_off = (len(refs) - 3) // 2
    acc, parts, sqs, out = refs[0], refs[1 : 1 + n_off], refs[1 + n_off : 2 + 2 * n_off], refs[-1]
    head = acc.shape[1] // 2
    inv = inverse_rms(sqs, full_width)
    out[...] = jnp.zeros_like(out)
    for b in range(acc.shape[0] // LANES):
        rows = pl.ds(b * LANES, LANES)
        v = acc[rows, head:]
        for p in parts:
            v = v + p[rows, :].astype(F32)
        total = to_lanes(jnp.sum(jnp.abs(v), axis=1, keepdims=True))
        out[b : b + 1, :] = total * (1.0 / head) * inv[b : b + 1, :]


def widen(column, below, above, lane, halfspan):
    pooled = column
    for shift in range(1, REACH + 1):
        right = pltpu.roll(jnp.where(lane < shift, below, column), LANES - shift, 1)
        left = pltpu.roll(jnp.where(lane >= LANES - shift, above, column), shift, 1)
        pooled = jnp.where(
            shift <= halfspan, jnp.maximum(jnp.maximum(pooled, right), left), pooled
        )
    return pooled


def pool_kernel(reach, got, mine, expo, vmag, used, spread):
    tok = expo.shape[0]
    nb = tok // LANES
    row_top = got[0, 0:1, :]
    for d in range(1, got.shape[0]):
        row_top = jnp.maximum(row_top, got[d, 0:1, :])
    row_total = jnp.zeros_like(row_top)
    for d in range(got.shape[0]):
        row_total = row_total + got[d, 1:2, :] * jnp.exp(got[d, 0:1, :] - row_top)
    weight = used[...] * jnp.exp(mine[0, 0:1, :] - row_top) / row_total
    height = vmag.shape[0]
    line = iota((height, LANES), 0)
    lane = iota((height, LANES), 1)
    column = jnp.zeros((height, LANES), F32)
    for b in range(nb):
        mass = jnp.sum(expo[b * LANES : (b + 1) * LANES, :] * weight, axis=1, keepdims=True)
        column = jnp.where(line == b, jnp.broadcast_to(to_lanes(mass), (height, LANES)), column)
    column = column * vmag[...]
    below, above = pltpu.roll(column, height - 1, 0), pltpu.roll(column, 1, 0)
    pooled = widen(column, below, above, lane, reach[...])
    place = line * LANES + lane
    inner = (place >= REACH) & (place < tok - REACH)
    sums = to_lanes(jnp.sum(jnp.where(inner, pooled, 0.0), axis=1, keepdims=True))
    flat = lane[0:1, :]
    last = pltpu.roll(column[nb - 1 : nb, :], 2 * EDGE, 1)
    said = jnp.where(flat < EDGE, column[0:1, :], jnp.where(flat < 2 * EDGE, last, pltpu.roll(sums, 2 * EDGE, 1)))
    spread[...] = jnp.broadcast_to(said, spread.shape)


def rank_kernel(nb, keep, reach, here, said, blocks, share):
    v = said[...]
    n = v.shape[0]
    line, lane = iota(v.shape, 0), iota(v.shape, 1)
    following = pltpu.roll(v, n - 1, 0)
    seam = jnp.where(lane < EDGE, pltpu.roll(v, LANES - EDGE, 1), pltpu.roll(following, EDGE, 1))
    seam = jnp.where(lane < 2 * EDGE, seam, 0.0)
    end = line == n - 1
    apart = LANES // 2
    both = jnp.where(end & (lane >= EDGE), 0.0, seam) + pltpu.roll(
        jnp.where(end & (lane < EDGE), 0.0, seam), apart, 1
    )
    pooled = both
    for shift in range(1, REACH + 1):
        near = jnp.maximum(pltpu.roll(both, shift, 1), pltpu.roll(both, LANES - shift, 1))
        pooled = jnp.where(shift <= reach[...], jnp.maximum(pooled, near), pooled)
    tail = (lane >= EDGE - REACH) & (lane < EDGE)
    lead = (lane >= apart + EDGE) & (lane < apart + EDGE + REACH)
    tail = jnp.sum(jnp.where(tail, pooled, 0.0), axis=1, keepdims=True)
    lead = jnp.sum(jnp.where(lead, pooled, 0.0), axis=1, keepdims=True)
    lead = pltpu.roll(jnp.broadcast_to(lead, v.shape), 1, 0)
    b = pltpu.roll(v, LANES - 2 * EDGE, 1)
    b = b + jnp.where(lane == 0, lead, 0.0) + jnp.where(lane == nb - 1, tail, 0.0)
    b = jnp.where(lane < nb, b, 0.0)
    own = jnp.sum(jnp.where(line == here[...], b, 0.0), axis=0, keepdims=True)
    blocks[...] = own[:, :nb]
    place = line * nb + lane
    rank = jnp.zeros(v.shape, jnp.int32)

    def turned(t, k):
        return jnp.where(lane >= k, pltpu.roll(t, k, 1), pltpu.roll(t, LANES + k - nb, 1)) if k else t

    for k in range(nb):
        bk, pk = turned(b, k), turned(place, k)
        for m in range(n):
            bm, pm = (pltpu.roll(bk, m, 0), pltpu.roll(pk, m, 0)) if m else (bk, pk)
            rank = rank + jnp.where((bm > b) | ((bm == b) & (pm < place)), 1, 0)

    def add(t):
        return jnp.sum(jnp.sum(t, axis=1, keepdims=True), axis=0, keepdims=True)

    kept = jnp.where((lane < nb) & (rank < keep[...]), b, 0.0)
    share[...] = add(kept) / add(b)


def local(
    hidden, gain, key_matrix, value_matrix, queries, window_len, kernel_width, kept_block_count
):
    tok, feats = hidden.shape
    full_width = gain.shape[0]
    head = key_matrix.shape[1]
    n_seq, n_head = lax.axis_size("seq"), lax.axis_size("head")
    n_x = n_head // CORES
    s, h = lax.axis_index("seq"), lax.axis_index("head")
    x, c = h // CORES, h % CORES
    i = s % GROUP
    q = feats // GROUP
    total_tokens = tok * n_seq
    offsets = range(1, n_x)

    def shift_x(offset):
        return [
            (a * CORES + b, (a + offset) % n_x * CORES + b) for a in range(n_x) for b in range(CORES)
        ]

    def flip(bit):
        return [(j, j ^ bit) for j in range(n_seq)]

    def rows_at(start, count):
        return [lax.dynamic_slice_in_dim(m, start, count) for m in (key_matrix, value_matrix)]

    def crossing(block):
        return [
            [
                rows_at(((x - o) % n_x * CORES + (c ^ part)) * feats + block * q, q)
                for part in range(CORES)
            ]
            for o in offsets
        ]

    def cross(rows):
        return [
            [
                [lax.ppermute(rows[o - 1][part][side], "head", shift_x(-o)) for side in range(2)]
                for part in range(CORES)
            ]
            for o in offsets
        ]

    lead = crossing(i)
    lead[0][0], key_matrix, value_matrix = lax.optimization_barrier(
        (lead[0][0], key_matrix, value_matrix)
    )
    rest = crossing(i)
    rest[0][0] = lead[0][0]
    firsts = cross(rest)
    seconds = cross(crossing(3 - i))
    own = [rows_at(start * feats, feats) for start in (h, h ^ 1)]
    swapped = lax.ppermute(hidden, "head", [(j, j ^ 1) for j in range(n_head)])
    blocks = [
        [
            [firsts[o - 1][part]]
            + [
                [lax.ppermute(firsts[o - 1][part][side], "seq", flip(bit)) for side in range(2)]
                for bit in (1, 2)
            ]
            + [seconds[o - 1][part]]
            for part in range(CORES)
        ]
        for o in offsets
    ]

    lines = -(-(tok // LANES) // 8) * 8
    gain_lines = gain.reshape(full_width // LANES, LANES)

    def norm(core, rows, own, more):
        return call(
            norm_kernel,
            [sds((tok, feats), BF16), sds((lines, LANES), F32), sds((tok, 2 * head), F32)],
            [SMEM] + [VMEM] * (4 + len(more)),
            flops=1 << 30,
        )(jnp.stack([core * (feats // LANES), i]), rows, gain_lines, *own, *more)

    mine, sumsq, acc = norm(h, hidden, own[0], ())

    window = queries.shape[0]
    group_heads = queries.shape[1] // head
    rows = window * group_heads
    row_window = (jnp.arange(rows) % window).astype(jnp.int32)[None, :]
    room = total_tokens - window + row_window - (s * tok + tok - window)
    used = (row_window >= window - window_len[0]).astype(F32)
    reach = jnp.broadcast_to((kernel_width - 1) // 2, (1, LANES))
    keep = jnp.broadcast_to(kept_block_count, (1, LANES))
    here = jnp.broadcast_to(s, (1, LANES)).astype(jnp.int32)
    swapped, room, used, reach, keep, here = lax.optimization_barrier(
        (swapped, room, used, reach, keep, here)
    )
    other, sumsq, acc = norm(h ^ 1, swapped, own[1], (sumsq, acc))
    sqs = [sumsq] + [lax.ppermute(sumsq, "head", shift_x(o)) for o in offsets]

    parts_k, parts_v = [], []
    wide, thin = sds((tok, 2 * head), F32), sds((tok, head), BF16)
    for o in offsets:
        half_0, half_1 = blocks[o - 1]
        part = call(early_kernel, wide, [VMEM] * 6, flops=1 << 29)(
            mine, other, *half_0[0], *half_1[0]
        )
        part = call(middle_kernel, wide, [VMEM] * 8, flops=1 << 29)(
            mine, part, *sum(half_0[1:], [])
        )
        part_k, part_v = call(
            late_kernel, [thin, thin], [VMEM] * 8, flops=1 << 29
        )(other, part, *sum(half_1[1:], []))
        parts_k.append(lax.ppermute(part_k, "head", shift_x(o)))
        parts_v.append(lax.ppermute(part_v, "head", shift_x(o)))

    half = head // 2
    freq = 500000.0 ** (-(jnp.arange(half).astype(F32) * 2.0) / head)
    token = s * tok + jnp.arange(tok)
    angle = token.astype(F32)[:, None] * freq[None, :]
    cos, sin = jnp.cos(angle), jnp.sin(angle)
    cos = jnp.concatenate([cos, cos], axis=1)
    sin = jnp.concatenate([-sin, sin], axis=1)

    expo, stats = call(
        functools.partial(score_kernel, full_width, head ** (-0.5)),
        [sds((tok, rows), F32), sds((n_seq, 2, rows), F32)],
        [VMEM] * (6 + 2 * len(offsets)),
        scratch=[pltpu.VMEM((tok, head), BF16), pltpu.VMEM((rows, head), BF16)],
        flops=1 << 28,
    )(acc, *parts_k, *sqs, cos, sin, queries, room)
    got = lax.all_to_all(stats, "seq", 0, 0, tiled=True)
    nb = tok // BLK
    vmag = call(
        functools.partial(value_kernel, full_width),
        sds((lines, LANES), F32),
        [VMEM] * (2 + 2 * len(offsets)),
        flops=1 << 28,
    )(acc, *parts_v, *sqs)
    spread = call(
        pool_kernel, sds((n_seq, LANES), F32), [VMEM] * 6, flops=1 << 26
    )(reach, got, stats, expo, vmag, used)
    said = lax.all_to_all(spread, "seq", 0, 0, tiled=True)
    local_blocks, fraction = call(
        functools.partial(rank_kernel, nb),
        [sds((1, nb), F32), sds((1, 1), F32)],
        [VMEM] * 4,
        flops=1 << 20,
    )(keep, reach, here, said)
    return (local_blocks, fraction.reshape(1))


def solution(mesh):
    return jax.shard_map(
        local,
        mesh=mesh,
        in_specs=(
            P("seq", "head"),
            P(),
            P(None, "head"),
            P(None, "head"),
            P(None, "head"),
            P("head"),
            P("head"),
            P("head"),
        ),
        out_specs=(P("head", "seq"), P("head")),
        check_vma=False,
    )
```

```python
import functools

import jax
import jax.numpy as jnp
from jax import lax
from jax.experimental import pallas as pl
from jax.experimental.pallas import tpu as pltpu
from jax.sharding import PartitionSpec as P

BLK = 128
LANES = 128
KERNEL_LIMIT = 15
REACH = (KERNEL_LIMIT - 1) // 2
EDGE = 16
CORES = 2
GROUP = 4
MASKED = -1e30

VMEM = pl.BlockSpec(memory_space=pltpu.VMEM)
SMEM = pl.BlockSpec(memory_space=pltpu.SMEM)
F32, BF16 = jnp.float32, jnp.bfloat16


def sds(shape, dtype):
    return jax.ShapeDtypeStruct(shape, dtype)


def call(body, out, ins, scratch=(), outs=None, flops=1 << 20, limit=40 << 20):
    return pl.pallas_call(
        body,
        out_shape=out,
        in_specs=ins,
        out_specs=outs if outs is not None else jax.tree.map(lambda _: VMEM, out),
        scratch_shapes=list(scratch),
        cost_estimate=pl.CostEstimate(flops=flops, bytes_accessed=1 << 20, transcendentals=0),
        compiler_params=pltpu.CompilerParams(vmem_limit_bytes=limit),
    )


def iota(shape, dim):
    return lax.broadcasted_iota(jnp.int32, shape, dim)


def to_lanes(col):
    n = col.shape[0]
    here = iota((n, LANES), 0) == iota((n, LANES), 1)
    return jnp.sum(jnp.where(here, jnp.broadcast_to(col, (n, LANES)), 0.0), axis=0, keepdims=True)


def to_rows(row, n):
    here = iota((n, LANES), 0) == iota((n, LANES), 1)
    return jnp.sum(jnp.where(here, jnp.broadcast_to(row, (n, LANES)), 0.0), axis=1, keepdims=True)


def norm_kernel(flip, hid, gain, weights, *refs):
    more = refs[:-3]
    normed, sumsq, acc = refs[-3:]
    tok, feats = hid.shape
    line = (lax.axis_index("head") ^ flip) * (feats // LANES)
    sumsq[...] = more[0][...] if more else jnp.zeros_like(sumsq)
    for b in range(tok // LANES):
        rows = pl.ds(b * LANES, LANES)
        folded = None
        for t in range(feats // LANES):
            lanes = pl.ds(t * LANES, LANES)
            raw = hid[rows, lanes].astype(F32)
            folded = raw * raw if folded is None else folded + raw * raw
            normed[rows, lanes] = (raw * gain[pl.ds(line + t, 1), :]).astype(BF16)
        sumsq[b : b + 1, :] += to_lanes(jnp.sum(folded, axis=1, keepdims=True))
    out = jnp.dot(normed[...], weights[...], preferred_element_type=F32)
    acc[...] = out + more[1][...] if more else out


def part_of(k, rows, blk):
    q = blk.shape[0]
    at = (lax.axis_index("seq") % GROUP) ^ k
    cols = pl.ds(pl.multiple_of(at * q, LANES), q)
    return jnp.dot(rows[:, cols], blk[...], preferred_element_type=F32)


def early_kernel(mine, other, a0, b0, out):
    out[...] = part_of(0, mine, a0) + part_of(0, other, b0)


def middle_kernel(mine, total, a1, a2, a3, out):
    acc = total[...]
    for k, blk in enumerate((a1, a2, a3)):
        acc = acc + part_of(k + 1, mine, blk)
    out[...] = acc


def late_kernel(other, total, b1, b2, b3, out_k, out_v):
    head = out_k.shape[1]
    acc = total[...]
    for k, blk in enumerate((b1, b2, b3)):
        acc = acc + part_of(k + 1, other, blk)
    out_k[...] = acc[:, :head].astype(BF16)
    out_v[...] = acc[:, head:].astype(BF16)


def inverse_rms(sqs, full_width):
    sumsq = sqs[0][...]
    for sq in sqs[1:]:
        sumsq = sumsq + sq[...]
    return lax.rsqrt(sumsq / full_width + 1e-05)


def score_kernel(full_width, scale_by, *refs):
    n_off = (len(refs) - 10) // 2
    acc, parts, sqs = refs[0], refs[1 : 1 + n_off], refs[1 + n_off : 2 + 2 * n_off]
    cos, sin, q, room, expo, stats, keys, rows_of = refs[2 + 2 * n_off :]
    tok, head = keys.shape
    window = q.shape[0]
    for j in range(q.shape[1] // head):
        rows_of[j * window : (j + 1) * window, :] = q[:, j * head : (j + 1) * head]
    inv = inverse_rms(sqs, full_width)
    for b in range(tok // LANES):
        rows = pl.ds(b * LANES, LANES)
        k = acc[rows, :head]
        for p in parts:
            k = k + p[rows, :].astype(F32)
        k = k * to_rows(inv[b : b + 1, :], LANES)
        keys[rows, :] = (k * cos[rows, :] + pltpu.roll(k, head // 2, 1) * sin[rows, :]).astype(BF16)
    scores = lax.dot_general(
        keys[...], rows_of[...], (((1,), (1,)), ((), ())), preferred_element_type=F32
    ) * scale_by
    open_to = tok - window
    tail = jnp.where(iota((window, 1), 0) <= room[...], scores[open_to:, :], MASKED)
    body = scores[:open_to, :]
    top = jnp.maximum(
        jnp.max(body, axis=0, keepdims=True), jnp.max(tail, axis=0, keepdims=True)
    )
    body, tail = jnp.exp(body - top), jnp.exp(tail - top)
    expo[:open_to, :] = body
    expo[open_to:, :] = tail
    own = jnp.sum(body, axis=0, keepdims=True) + jnp.sum(tail, axis=0, keepdims=True)
    for d in range(stats.shape[0]):
        stats[d, 0:1, :] = top
        stats[d, 1:2, :] = own


def value_kernel(full_width, *refs):
    n_off = (len(refs) - 3) // 2
    acc, parts, sqs, out = refs[0], refs[1 : 1 + n_off], refs[1 + n_off : 2 + 2 * n_off], refs[-1]
    head = acc.shape[1] // 2
    inv = inverse_rms(sqs, full_width)
    out[...] = jnp.zeros_like(out)
    for b in range(acc.shape[0] // LANES):
        rows = pl.ds(b * LANES, LANES)
        v = acc[rows, head:]
        for p in parts:
            v = v + p[rows, :].astype(F32)
        total = to_lanes(jnp.sum(jnp.abs(v), axis=1, keepdims=True))
        out[b : b + 1, :] = total * (1.0 / head) * inv[b : b + 1, :]


def widen(column, below, above, lane, halfspan):
    pooled = column
    for shift in range(1, REACH + 1):
        right = pltpu.roll(jnp.where(lane < shift, below, column), LANES - shift, 1)
        left = pltpu.roll(jnp.where(lane >= LANES - shift, above, column), shift, 1)
        pooled = jnp.where(
            shift <= halfspan, jnp.maximum(jnp.maximum(pooled, right), left), pooled
        )
    return pooled


def pool_kernel(reach, got, mine, expo, vmag, used, spread):
    tok = expo.shape[0]
    nb = tok // LANES
    row_top = got[0, 0:1, :]
    for d in range(1, got.shape[0]):
        row_top = jnp.maximum(row_top, got[d, 0:1, :])
    row_total = jnp.zeros_like(row_top)
    for d in range(got.shape[0]):
        row_total = row_total + got[d, 1:2, :] * jnp.exp(got[d, 0:1, :] - row_top)
    weight = used[...] * jnp.exp(mine[0, 0:1, :] - row_top) / row_total
    height = vmag.shape[0]
    line = iota((height, LANES), 0)
    lane = iota((height, LANES), 1)
    column = jnp.zeros((height, LANES), F32)
    for b in range(nb):
        mass = jnp.sum(expo[b * LANES : (b + 1) * LANES, :] * weight, axis=1, keepdims=True)
        column = jnp.where(line == b, jnp.broadcast_to(to_lanes(mass), (height, LANES)), column)
    column = column * vmag[...]
    below, above = pltpu.roll(column, height - 1, 0), pltpu.roll(column, 1, 0)
    pooled = widen(column, below, above, lane, reach[...])
    place = line * LANES + lane
    inner = (place >= REACH) & (place < tok - REACH)
    sums = to_lanes(jnp.sum(jnp.where(inner, pooled, 0.0), axis=1, keepdims=True))
    flat = lane[0:1, :]
    last = pltpu.roll(column[nb - 1 : nb, :], 2 * EDGE, 1)
    said = jnp.where(flat < EDGE, column[0:1, :], jnp.where(flat < 2 * EDGE, last, pltpu.roll(sums, 2 * EDGE, 1)))
    spread[...] = jnp.broadcast_to(said, spread.shape)


def rank_kernel(nb, keep, reach, here, said, blocks, share):
    v = said[...]
    n = v.shape[0]
    line, lane = iota(v.shape, 0), iota(v.shape, 1)
    following = pltpu.roll(v, n - 1, 0)
    seam = jnp.where(lane < EDGE, pltpu.roll(v, LANES - EDGE, 1), pltpu.roll(following, EDGE, 1))
    seam = jnp.where(lane < 2 * EDGE, seam, 0.0)
    end = line == n - 1
    apart = LANES // 2
    both = jnp.where(end & (lane >= EDGE), 0.0, seam) + pltpu.roll(
        jnp.where(end & (lane < EDGE), 0.0, seam), apart, 1
    )
    pooled = both
    for shift in range(1, REACH + 1):
        near = jnp.maximum(pltpu.roll(both, shift, 1), pltpu.roll(both, LANES - shift, 1))
        pooled = jnp.where(shift <= reach[...], jnp.maximum(pooled, near), pooled)
    tail = (lane >= EDGE - REACH) & (lane < EDGE)
    lead = (lane >= apart + EDGE) & (lane < apart + EDGE + REACH)
    tail = jnp.sum(jnp.where(tail, pooled, 0.0), axis=1, keepdims=True)
    lead = jnp.sum(jnp.where(lead, pooled, 0.0), axis=1, keepdims=True)
    lead = pltpu.roll(jnp.broadcast_to(lead, v.shape), 1, 0)
    b = pltpu.roll(v, LANES - 2 * EDGE, 1)
    b = b + jnp.where(lane == 0, lead, 0.0) + jnp.where(lane == nb - 1, tail, 0.0)
    b = jnp.where(lane < nb, b, 0.0)
    own = jnp.sum(jnp.where(line == here[...], b, 0.0), axis=0, keepdims=True)
    blocks[...] = own[:, :nb]
    place = line * nb + lane
    rank = jnp.zeros(v.shape, jnp.int32)

    def turned(t, k):
        return jnp.where(lane >= k, pltpu.roll(t, k, 1), pltpu.roll(t, LANES + k - nb, 1)) if k else t

    for k in range(nb):
        bk, pk = turned(b, k), turned(place, k)
        for m in range(n):
            bm, pm = (pltpu.roll(bk, m, 0), pltpu.roll(pk, m, 0)) if m else (bk, pk)
            rank = rank + jnp.where((bm > b) | ((bm == b) & (pm < place)), 1, 0)

    def add(t):
        return jnp.sum(jnp.sum(t, axis=1, keepdims=True), axis=0, keepdims=True)

    kept = jnp.where((lane < nb) & (rank < keep[...]), b, 0.0)
    share[...] = add(kept) / add(b)


def local(
    hidden, gain, key_matrix, value_matrix, queries, window_len, kernel_width, kept_block_count
):
    tok, feats = hidden.shape
    full_width = gain.shape[0]
    head = key_matrix.shape[1]
    n_seq, n_head = lax.axis_size("seq"), lax.axis_size("head")
    n_x = n_head // CORES
    s, h = lax.axis_index("seq"), lax.axis_index("head")
    x, c = h // CORES, h % CORES
    i = s % GROUP
    q = feats // GROUP
    total_tokens = tok * n_seq
    offsets = range(1, n_x)

    def shift_x(offset):
        return [
            (a * CORES + b, (a + offset) % n_x * CORES + b) for a in range(n_x) for b in range(CORES)
        ]

    def flip(bit):
        return [(j, j ^ bit) for j in range(n_seq)]

    def sides_at(start, count):
        return [lax.dynamic_slice_in_dim(m, start, count) for m in (key_matrix, value_matrix)]

    def rows_at(start, count):
        return jnp.concatenate(sides_at(start, count), axis=1)

    def row_of(o, part, block):
        return ((x - o) % n_x * CORES + (c ^ part)) * feats + block * q

    def cross(o, rows):
        return lax.ppermute(rows, "head", shift_x(-o))

    lead = sides_at(row_of(1, 0, i), q)
    lead, key_matrix, value_matrix = lax.optimization_barrier((lead, key_matrix, value_matrix))
    lead = [lax.ppermute(rows, "head", shift_x(-1)) for rows in lead]
    firsts = [
        [
            jnp.concatenate(lead, axis=1)
            if (o, part) == (1, 0)
            else cross(o, rows_at(row_of(o, part, i), q))
            for part in range(CORES)
        ]
        for o in offsets
    ]
    seconds = [
        [cross(o, rows_at(row_of(o, part, 3 - i), q)) for part in range(CORES)]
        for o in offsets
    ]
    own = [rows_at(start * feats, feats) for start in (h, h ^ 1)]
    swapped = lax.ppermute(hidden, "head", [(j, j ^ 1) for j in range(n_head)])
    blocks = [
        [
            [firsts[o - 1][part]]
            + [lax.ppermute(firsts[o - 1][part], "seq", flip(bit)) for bit in (1, 2)]
            + [seconds[o - 1][part]]
            for part in range(CORES)
        ]
        for o in offsets
    ]

    lines = -(-(tok // LANES) // 8) * 8
    gain_lines = gain.reshape(full_width // LANES, LANES)

    def norm(flip, rows, own, more):
        return call(
            functools.partial(norm_kernel, flip),
            [sds((tok, feats), BF16), sds((lines, LANES), F32), sds((tok, 2 * head), F32)],
            [VMEM] * (3 + len(more)),
            flops=1 << 30,
        )(rows, gain_lines, own, *more)

    mine, sumsq, acc = norm(0, hidden, own[0], ())

    window = queries.shape[0]
    group_heads = queries.shape[1] // head
    rows = window * group_heads
    row_window = (jnp.arange(rows) % window).astype(jnp.int32)[None, :]
    room = total_tokens - window + row_window - (s * tok + tok - window)
    used = (row_window >= window - window_len[0]).astype(F32)
    reach = jnp.broadcast_to((kernel_width - 1) // 2, (1, LANES))
    keep = jnp.broadcast_to(kept_block_count, (1, LANES))
    here = jnp.broadcast_to(s, (1, LANES)).astype(jnp.int32)
    swapped, room, used, reach, keep, here = lax.optimization_barrier(
        (swapped, room, used, reach, keep, here)
    )
    other, sumsq, acc = norm(1, swapped, own[1], (sumsq, acc))
    sqs = [sumsq] + [lax.ppermute(sumsq, "head", shift_x(o)) for o in offsets]

    parts_k, parts_v = [], []
    wide, thin = sds((tok, 2 * head), F32), sds((tok, head), BF16)
    for o in offsets:
        half_0, half_1 = blocks[o - 1]
        part = call(early_kernel, wide, [VMEM] * 4, flops=1 << 29)(
            mine, other, half_0[0], half_1[0]
        )
        part = call(middle_kernel, wide, [VMEM] * 5, flops=1 << 29)(mine, part, *half_0[1:])
        part_k, part_v = call(
            late_kernel, [thin, thin], [VMEM] * 5, flops=1 << 29
        )(other, part, *half_1[1:])
        parts_k.append(lax.ppermute(part_k, "head", shift_x(o)))
        parts_v.append(lax.ppermute(part_v, "head", shift_x(o)))

    half = head // 2
    freq = 500000.0 ** (-(jnp.arange(half).astype(F32) * 2.0) / head)
    token = s * tok + jnp.arange(tok)
    angle = token.astype(F32)[:, None] * freq[None, :]
    cos, sin = jnp.cos(angle), jnp.sin(angle)
    cos = jnp.concatenate([cos, cos], axis=1)
    sin = jnp.concatenate([-sin, sin], axis=1)

    expo, stats = call(
        functools.partial(score_kernel, full_width, head ** (-0.5)),
        [sds((tok, rows), F32), sds((n_seq, 2, rows), F32)],
        [VMEM] * (6 + 2 * len(offsets)),
        scratch=[pltpu.VMEM((tok, head), BF16), pltpu.VMEM((rows, head), BF16)],
        flops=1 << 28,
    )(acc, *parts_k, *sqs, cos, sin, queries, room)
    got = lax.all_to_all(stats, "seq", 0, 0, tiled=True)
    nb = tok // BLK
    vmag = call(
        functools.partial(value_kernel, full_width),
        sds((lines, LANES), F32),
        [VMEM] * (2 + 2 * len(offsets)),
        flops=1 << 28,
    )(acc, *parts_v, *sqs)
    spread = call(
        pool_kernel, sds((n_seq, LANES), F32), [VMEM] * 6, flops=1 << 26
    )(reach, got, stats, expo, vmag, used)
    said = lax.all_to_all(spread, "seq", 0, 0, tiled=True)
    local_blocks, fraction = call(
        functools.partial(rank_kernel, nb),
        [sds((1, nb), F32), sds((1, 1), F32)],
        [VMEM] * 4,
        flops=1 << 20,
    )(keep, reach, here, said)
    return (local_blocks, fraction.reshape(1))


def solution(mesh):
    return jax.shard_map(
        local,
        mesh=mesh,
        in_specs=(
            P("seq", "head"),
            P(),
            P(None, "head"),
            P(None, "head"),
            P(None, "head"),
            P("head"),
            P("head"),
            P("head"),
        ),
        out_specs=(P("head", "seq"), P("head")),
        check_vma=False,
    )
```

```python
import functools

import jax
import jax.numpy as jnp
from jax import lax
from jax.experimental import pallas as pl
from jax.experimental.pallas import tpu as pltpu
from jax.sharding import PartitionSpec as P

BLK = 128
LANES = 128
KERNEL_LIMIT = 15
REACH = (KERNEL_LIMIT - 1) // 2
EDGE = 16
CORES = 2
GROUP = 4
MASKED = -1e30

VMEM = pl.BlockSpec(memory_space=pltpu.VMEM)
SMEM = pl.BlockSpec(memory_space=pltpu.SMEM)
F32, BF16 = jnp.float32, jnp.bfloat16


def sds(shape, dtype):
    return jax.ShapeDtypeStruct(shape, dtype)


def call(body, out, ins, scratch=(), outs=None, flops=1 << 20, limit=40 << 20):
    return pl.pallas_call(
        body,
        out_shape=out,
        in_specs=ins,
        out_specs=outs if outs is not None else jax.tree.map(lambda _: VMEM, out),
        scratch_shapes=list(scratch),
        cost_estimate=pl.CostEstimate(flops=flops, bytes_accessed=1 << 20, transcendentals=0),
        compiler_params=pltpu.CompilerParams(vmem_limit_bytes=limit),
    )


def iota(shape, dim):
    return lax.broadcasted_iota(jnp.int32, shape, dim)


def to_lanes(col):
    n = col.shape[0]
    here = iota((n, LANES), 0) == iota((n, LANES), 1)
    return jnp.sum(jnp.where(here, jnp.broadcast_to(col, (n, LANES)), 0.0), axis=0, keepdims=True)


def to_rows(row, n):
    here = iota((n, LANES), 0) == iota((n, LANES), 1)
    return jnp.sum(jnp.where(here, jnp.broadcast_to(row, (n, LANES)), 0.0), axis=1, keepdims=True)


def norm_kernel(flip, hid, gain, weights, *refs):
    more = refs[:-3]
    normed, sumsq, acc = refs[-3:]
    tok, feats = hid.shape
    line = (lax.axis_index("head") ^ flip) * (feats // LANES)
    sumsq[...] = more[0][...] if more else jnp.zeros_like(sumsq)
    for b in range(tok // LANES):
        rows = pl.ds(b * LANES, LANES)
        folded = None
        for t in range(feats // LANES):
            lanes = pl.ds(t * LANES, LANES)
            raw = hid[rows, lanes].astype(F32)
            folded = raw * raw if folded is None else folded + raw * raw
            normed[rows, lanes] = (raw * gain[pl.ds(line + t, 1), :]).astype(BF16)
        sumsq[b : b + 1, :] += to_lanes(jnp.sum(folded, axis=1, keepdims=True))
    out = jnp.dot(normed[...], weights[...], preferred_element_type=F32)
    acc[...] = out + more[1][...] if more else out


def part_of(k, rows, blk):
    q = blk.shape[0]
    at = (lax.axis_index("seq") % GROUP) ^ k
    cols = pl.ds(pl.multiple_of(at * q, LANES), q)
    return jnp.dot(rows[:, cols], blk[...], preferred_element_type=F32)


def early_kernel(mine, other, a0, b0, out):
    out[...] = part_of(0, mine, a0) + part_of(0, other, b0)


def middle_kernel(mine, total, a1, a2, a3, out):
    acc = total[...]
    for k, blk in enumerate((a1, a2, a3)):
        acc = acc + part_of(k + 1, mine, blk)
    out[...] = acc


def late_kernel(other, total, b1, b2, b3, out_k, out_v):
    head = out_k.shape[1]
    acc = total[...]
    for k, blk in enumerate((b1, b2, b3)):
        acc = acc + part_of(k + 1, other, blk)
    out_k[...] = acc[:, :head].astype(BF16)
    out_v[...] = acc[:, head:].astype(BF16)


def inverse_rms(sqs, full_width):
    sumsq = sqs[0][...]
    for sq in sqs[1:]:
        sumsq = sumsq + sq[...]
    return lax.rsqrt(sumsq / full_width + 1e-05)


def score_kernel(full_width, scale_by, *refs):
    n_off = (len(refs) - 10) // 2
    acc, parts, sqs = refs[0], refs[1 : 1 + n_off], refs[1 + n_off : 2 + 2 * n_off]
    cos, sin, q, room, expo, stats, keys, rows_of = refs[2 + 2 * n_off :]
    tok, head = keys.shape
    window = q.shape[0]
    for j in range(q.shape[1] // head):
        rows_of[j * window : (j + 1) * window, :] = q[:, j * head : (j + 1) * head]
    inv = inverse_rms(sqs, full_width)
    for b in range(tok // LANES):
        rows = pl.ds(b * LANES, LANES)
        k = acc[rows, :head]
        for p in parts:
            k = k + p[rows, :].astype(F32)
        k = k * to_rows(inv[b : b + 1, :], LANES)
        keys[rows, :] = (k * cos[rows, :] + pltpu.roll(k, head // 2, 1) * sin[rows, :]).astype(BF16)
    scores = lax.dot_general(
        keys[...], rows_of[...], (((1,), (1,)), ((), ())), preferred_element_type=F32
    ) * scale_by
    open_to = tok - window
    tail = jnp.where(iota((window, 1), 0) <= room[...], scores[open_to:, :], MASKED)
    body = scores[:open_to, :]
    top = jnp.maximum(
        jnp.max(body, axis=0, keepdims=True), jnp.max(tail, axis=0, keepdims=True)
    )
    body, tail = jnp.exp(body - top), jnp.exp(tail - top)
    expo[:open_to, :] = body
    expo[open_to:, :] = tail
    own = jnp.sum(body, axis=0, keepdims=True) + jnp.sum(tail, axis=0, keepdims=True)
    for d in range(stats.shape[0]):
        stats[d, 0:1, :] = top
        stats[d, 1:2, :] = own


def value_kernel(full_width, *refs):
    n_off = (len(refs) - 3) // 2
    acc, parts, sqs, out = refs[0], refs[1 : 1 + n_off], refs[1 + n_off : 2 + 2 * n_off], refs[-1]
    head = acc.shape[1] // 2
    inv = inverse_rms(sqs, full_width)
    out[...] = jnp.zeros_like(out)
    for b in range(acc.shape[0] // LANES):
        rows = pl.ds(b * LANES, LANES)
        v = acc[rows, head:]
        for p in parts:
            v = v + p[rows, :].astype(F32)
        total = to_lanes(jnp.sum(jnp.abs(v), axis=1, keepdims=True))
        out[b : b + 1, :] = total * (1.0 / head) * inv[b : b + 1, :]


def widen(column, below, above, lane, halfspan):
    pooled = column
    for shift in range(1, REACH + 1):
        right = pltpu.roll(jnp.where(lane < shift, below, column), LANES - shift, 1)
        left = pltpu.roll(jnp.where(lane >= LANES - shift, above, column), shift, 1)
        pooled = jnp.where(
            shift <= halfspan, jnp.maximum(jnp.maximum(pooled, right), left), pooled
        )
    return pooled


def pool_kernel(reach, got, mine, expo, vmag, used, spread):
    tok = expo.shape[0]
    nb = tok // LANES
    row_top = got[0, 0:1, :]
    for d in range(1, got.shape[0]):
        row_top = jnp.maximum(row_top, got[d, 0:1, :])
    row_total = jnp.zeros_like(row_top)
    for d in range(got.shape[0]):
        row_total = row_total + got[d, 1:2, :] * jnp.exp(got[d, 0:1, :] - row_top)
    weight = used[...] * jnp.exp(mine[0, 0:1, :] - row_top) / row_total
    height = vmag.shape[0]
    line = iota((height, LANES), 0)
    lane = iota((height, LANES), 1)
    column = jnp.zeros((height, LANES), F32)
    for b in range(nb):
        mass = jnp.sum(expo[b * LANES : (b + 1) * LANES, :] * weight, axis=1, keepdims=True)
        column = jnp.where(line == b, jnp.broadcast_to(to_lanes(mass), (height, LANES)), column)
    column = column * vmag[...]
    below, above = pltpu.roll(column, height - 1, 0), pltpu.roll(column, 1, 0)
    pooled = widen(column, below, above, lane, reach[...])
    place = line * LANES + lane
    inner = (place >= REACH) & (place < tok - REACH)
    sums = to_lanes(jnp.sum(jnp.where(inner, pooled, 0.0), axis=1, keepdims=True))
    flat = lane[0:1, :]
    last = pltpu.roll(column[nb - 1 : nb, :], 2 * EDGE, 1)
    said = jnp.where(flat < EDGE, column[0:1, :], jnp.where(flat < 2 * EDGE, last, pltpu.roll(sums, 2 * EDGE, 1)))
    spread[...] = jnp.broadcast_to(said, spread.shape)


def rank_kernel(nb, keep, reach, here, said, blocks, share):
    v = said[...]
    n = v.shape[0]
    line, lane = iota(v.shape, 0), iota(v.shape, 1)
    following = pltpu.roll(v, n - 1, 0)
    seam = jnp.where(lane < EDGE, pltpu.roll(v, LANES - EDGE, 1), pltpu.roll(following, EDGE, 1))
    seam = jnp.where(lane < 2 * EDGE, seam, 0.0)
    end = line == n - 1
    apart = LANES // 2
    both = jnp.where(end & (lane >= EDGE), 0.0, seam) + pltpu.roll(
        jnp.where(end & (lane < EDGE), 0.0, seam), apart, 1
    )
    pooled = both
    for shift in range(1, REACH + 1):
        near = jnp.maximum(pltpu.roll(both, shift, 1), pltpu.roll(both, LANES - shift, 1))
        pooled = jnp.where(shift <= reach[...], jnp.maximum(pooled, near), pooled)
    tail = (lane >= EDGE - REACH) & (lane < EDGE)
    lead = (lane >= apart + EDGE) & (lane < apart + EDGE + REACH)
    tail = jnp.sum(jnp.where(tail, pooled, 0.0), axis=1, keepdims=True)
    lead = jnp.sum(jnp.where(lead, pooled, 0.0), axis=1, keepdims=True)
    lead = pltpu.roll(jnp.broadcast_to(lead, v.shape), 1, 0)
    b = pltpu.roll(v, LANES - 2 * EDGE, 1)
    b = b + jnp.where(lane == 0, lead, 0.0) + jnp.where(lane == nb - 1, tail, 0.0)
    b = jnp.where(lane < nb, b, 0.0)
    own = jnp.sum(jnp.where(line == here[...], b, 0.0), axis=0, keepdims=True)
    blocks[...] = own[:, :nb]
    place = line * nb + lane
    rank = jnp.zeros(v.shape, jnp.int32)

    def turned(t, k):
        return jnp.where(lane >= k, pltpu.roll(t, k, 1), pltpu.roll(t, LANES + k - nb, 1)) if k else t

    for k in range(nb):
        bk, pk = turned(b, k), turned(place, k)
        for m in range(n):
            bm, pm = (pltpu.roll(bk, m, 0), pltpu.roll(pk, m, 0)) if m else (bk, pk)
            rank = rank + jnp.where((bm > b) | ((bm == b) & (pm < place)), 1, 0)

    def add(t):
        return jnp.sum(jnp.sum(t, axis=1, keepdims=True), axis=0, keepdims=True)

    kept = jnp.where((lane < nb) & (rank < keep[...]), b, 0.0)
    share[...] = add(kept) / add(b)


def local(
    hidden, gain, key_matrix, value_matrix, queries, window_len, kernel_width, kept_block_count
):
    tok, feats = hidden.shape
    full_width = gain.shape[0]
    head = key_matrix.shape[1]
    n_seq, n_head = lax.axis_size("seq"), lax.axis_size("head")
    n_x = n_head // CORES
    s, h = lax.axis_index("seq"), lax.axis_index("head")
    x, c = h // CORES, h % CORES
    i = s % GROUP
    q = feats // GROUP
    total_tokens = tok * n_seq
    offsets = range(1, n_x)

    def shift_x(offset):
        return [
            (a * CORES + b, (a + offset) % n_x * CORES + b) for a in range(n_x) for b in range(CORES)
        ]

    def flip(bit):
        return [(j, j ^ bit) for j in range(n_seq)]

    def rows_at(start, count):
        return jnp.concatenate(
            [lax.dynamic_slice_in_dim(m, start, count) for m in (key_matrix, value_matrix)], axis=1
        )

    def crossing(block):
        return [
            [
                rows_at(((x - o) % n_x * CORES + (c ^ part)) * feats + block * q, q)
                for part in range(CORES)
            ]
            for o in offsets
        ]

    def cross(rows):
        return [
            [lax.ppermute(rows[o - 1][part], "head", shift_x(-o)) for part in range(CORES)]
            for o in offsets
        ]

    lead = crossing(i)
    lead[0][0], key_matrix, value_matrix = lax.optimization_barrier(
        (lead[0][0], key_matrix, value_matrix)
    )
    firsts = cross([lead[0][:1] + rest[1:] if k == 0 else rest for k, rest in enumerate(crossing(i))])
    seconds = cross(crossing(3 - i))
    own = [rows_at(start * feats, feats) for start in (h, h ^ 1)]
    swapped = lax.ppermute(hidden, "head", [(j, j ^ 1) for j in range(n_head)])
    blocks = [
        [
            [firsts[o - 1][part]]
            + [lax.ppermute(firsts[o - 1][part], "seq", flip(bit)) for bit in (1, 2)]
            + [seconds[o - 1][part]]
            for part in range(CORES)
        ]
        for o in offsets
    ]

    lines = -(-(tok // LANES) // 8) * 8
    gain_lines = gain.reshape(full_width // LANES, LANES)

    def norm(flip, rows, own, more):
        return call(
            functools.partial(norm_kernel, flip),
            [sds((tok, feats), BF16), sds((lines, LANES), F32), sds((tok, 2 * head), F32)],
            [VMEM] * (3 + len(more)),
            flops=1 << 30,
        )(rows, gain_lines, own, *more)

    mine, sumsq, acc = norm(0, hidden, own[0], ())

    window = queries.shape[0]
    group_heads = queries.shape[1] // head
    rows = window * group_heads
    row_window = (jnp.arange(rows) % window).astype(jnp.int32)[None, :]
    room = total_tokens - window + row_window - (s * tok + tok - window)
    used = (row_window >= window - window_len[0]).astype(F32)
    reach = jnp.broadcast_to((kernel_width - 1) // 2, (1, LANES))
    keep = jnp.broadcast_to(kept_block_count, (1, LANES))
    here = jnp.broadcast_to(s, (1, LANES)).astype(jnp.int32)
    swapped, room, used, reach, keep, here = lax.optimization_barrier(
        (swapped, room, used, reach, keep, here)
    )
    other, sumsq, acc = norm(1, swapped, own[1], (sumsq, acc))
    sqs = [sumsq] + [lax.ppermute(sumsq, "head", shift_x(o)) for o in offsets]

    parts_k, parts_v = [], []
    wide, thin = sds((tok, 2 * head), F32), sds((tok, head), BF16)
    for o in offsets:
        half_0, half_1 = blocks[o - 1]
        part = call(early_kernel, wide, [VMEM] * 4, flops=1 << 29)(
            mine, other, half_0[0], half_1[0]
        )
        part = call(middle_kernel, wide, [VMEM] * 5, flops=1 << 29)(mine, part, *half_0[1:])
        part_k, part_v = call(
            late_kernel, [thin, thin], [VMEM] * 5, flops=1 << 29
        )(other, part, *half_1[1:])
        parts_k.append(lax.ppermute(part_k, "head", shift_x(o)))
        parts_v.append(lax.ppermute(part_v, "head", shift_x(o)))

    half = head // 2
    freq = 500000.0 ** (-(jnp.arange(half).astype(F32) * 2.0) / head)
    token = s * tok + jnp.arange(tok)
    angle = token.astype(F32)[:, None] * freq[None, :]
    cos, sin = jnp.cos(angle), jnp.sin(angle)
    cos = jnp.concatenate([cos, cos], axis=1)
    sin = jnp.concatenate([-sin, sin], axis=1)

    expo, stats = call(
        functools.partial(score_kernel, full_width, head ** (-0.5)),
        [sds((tok, rows), F32), sds((n_seq, 2, rows), F32)],
        [VMEM] * (6 + 2 * len(offsets)),
        scratch=[pltpu.VMEM((tok, head), BF16), pltpu.VMEM((rows, head), BF16)],
        flops=1 << 28,
    )(acc, *parts_k, *sqs, cos, sin, queries, room)
    got = lax.all_to_all(stats, "seq", 0, 0, tiled=True)
    nb = tok // BLK
    vmag = call(
        functools.partial(value_kernel, full_width),
        sds((lines, LANES), F32),
        [VMEM] * (2 + 2 * len(offsets)),
        flops=1 << 28,
    )(acc, *parts_v, *sqs)
    spread = call(
        pool_kernel, sds((n_seq, LANES), F32), [VMEM] * 6, flops=1 << 26
    )(reach, got, stats, expo, vmag, used)
    said = lax.all_to_all(spread, "seq", 0, 0, tiled=True)
    local_blocks, fraction = call(
        functools.partial(rank_kernel, nb),
        [sds((1, nb), F32), sds((1, 1), F32)],
        [VMEM] * 4,
        flops=1 << 20,
    )(keep, reach, here, said)
    return (local_blocks, fraction.reshape(1))


def solution(mesh):
    return jax.shard_map(
        local,
        mesh=mesh,
        in_specs=(
            P("seq", "head"),
            P(),
            P(None, "head"),
            P(None, "head"),
            P(None, "head"),
            P("head"),
            P("head"),
            P("head"),
        ),
        out_specs=(P("head", "seq"), P("head")),
        check_vma=False,
    )
```
